32 devices in a mesh: seq: 8 (over z, x), tp: 4 (over y, core).
Axes of the slice: x: 2, y: 2, z: 4, core: 2. Of those that a mesh axis runs over, the one named last changes fastest.
Arguments:
- query_rows: bfloat16 [1536, 4096], P('seq', 'tp'), may hold values from -120 to 120
- key_rows: bfloat16 [1536, 1024], P('seq', 'tp'), may hold values from -6 to 6
- value_rows: bfloat16 [1536, 1024], P('seq', 'tp'), may hold values from -6 to 6
- document_ids: int32 [1536], replicated, may hold values from 0 to 3, never falling along the last dimension, each value on 1 to 768 neighbouring positions
- output_weight: bfloat16 [4096, 8192], P('tp'), may hold values from -0.09375 to 0.09375
Outputs:
- attended: bfloat16 [1536, 8192], P(('seq', 'tp'))
The draws below stay inside these ranges and needn't reach their ends.
Inputs may be any that keep to these rules, and one draw needn't show every extreme that they name: `document_ids`: never falling along the sequence; every document holds at most 768 tokens, and one holds exactly 768.
All inputs are finite; a program needn't handle non-finite values.
Results may differ from the reference program's by a relative error of at most 0.014.
Values may be sent and summed in bfloat16 or wider, within the bound.
No kernel may reach another device: no remote copies, remote signals or barrier semaphores. Data moves between devices by JAX's collectives and lax.ppermute only.
A program may use at most 64 MiB of HBM per device.

```python
import math
import jax
import jax.numpy as jnp
import numpy as np
from jax import lax

D = 8192
HEADS = 32
KV = 8
HD = 128
TOK_DEV = 192
SEQ = 1536
MAXDOC = 768
N_TP = 4


def query_key_pair(key):
    key_query, key_keys = jax.random.split(key, 2)
    keys_drawn = jnp.clip(jax.random.normal(key_keys, (SEQ, KV * HD), jnp.float32), -6.0, 6.0)
    queries = jnp.clip(jax.random.normal(key_query, (SEQ, HEADS * HD), jnp.float32), -6.0, 6.0)
    return (queries, keys_drawn)


def draw_query_rows(key, part):
    return query_key_pair(jax.random.fold_in(key, 11))[0].astype(jnp.bfloat16)


def draw_key_rows(key, part):
    return query_key_pair(jax.random.fold_in(key, 11))[1].astype(jnp.bfloat16)


def level_of(own_key, dims, cuts, least, top_value):
    def one(dim, shards_of):
        draws = jax.random.uniform(jax.random.fold_in(jax.random.fold_in(own_key, 6), dim), (shards_of,), jnp.float32, least / len(cuts), top_value / len(cuts))
        return jnp.repeat(jnp.exp(draws), dims[dim] // shards_of).reshape((-1,) + (1,) * (len(dims) - dim - 1))

    loudness = one(*cuts[0])
    for cut in cuts[1:]:
        loudness = loudness * one(*cut)
    return loudness


def length_profile(amount, total, most, slope):
    loads = [(1 << 20) // math.isqrt(grade ** slope) + 1 for grade in range(2, amount + 1)]
    rest, counts = total - most - (amount - 1), [1] * (amount - 1)
    while rest > 0:
        free = [i for i in range(amount - 1) if counts[i] < most]
        whole, remaining = sum([loads[i] for i in free]), rest
        for i in free:
            addition = min(most - counts[i], max(1, remaining * loads[i] // whole), rest)
            counts[i] = counts[i] + addition
            rest = rest - addition
    return np.array([most] + counts)


def ragged(key, amount, total, most, skew):
    if amount == 2:
        one = jax.random.randint(key, (), max(1, total - most), min(most, total - 1) + 1)
        return jnp.stack([one, total - one])
    sizes = jnp.asarray(length_profile(amount, total, most, skew), jnp.int32)
    twos = (amount - 1) // 2
    donor, receiver = sizes[1:1 + 2 * twos:2], sizes[2:2 + 2 * twos:2]
    room = jnp.minimum(donor - 1, most - receiver)
    shifted = jax.random.randint(jax.random.fold_in(key, 1), (twos,), 0, 1 << 20) % (room + 1)
    sizes = sizes.at[1:1 + 2 * twos:2].set(donor - shifted).at[2:2 + 2 * twos:2].set(receiver + shifted)
    return sizes[jax.random.permutation(jax.random.fold_in(key, 2), amount)]


def bell_draw(key, shape, scale, bound, shards=(), kind=jnp.bfloat16):
    gain = level_of(key, shape, shards, -0.22, 0.18) if shards else 1.0
    entries = jax.random.normal(key, shape, jnp.float32) * scale * gain
    return jnp.minimum(jnp.maximum(entries, -bound), bound).astype(kind)


def setup_inputs(seed: int = 0) -> dict:
    keys = jax.random.split(jax.random.key(seed), 6)
    query_rows = draw_query_rows(jax.random.fold_in(keys[5], 71), 0)
    key_rows = draw_key_rows(jax.random.fold_in(keys[5], 71), 0)
    value_rows = bell_draw(keys[2], (SEQ, KV * HD), 1.0, 6.0, ((0, 8), (1, 4)))
    document_ids = jnp.searchsorted(jnp.cumsum(ragged(keys[3], 2 * SEQ // MAXDOC, SEQ, MAXDOC, 2)), jnp.arange(SEQ), side="right").astype(jnp.int32)
    output_weight = bell_draw(keys[4], (HEADS * HD, D), (HEADS * HD) ** -0.5, 0.09375, ((0, 4),))
    return dict(query_rows=query_rows, key_rows=key_rows, value_rows=value_rows, document_ids=document_ids, output_weight=output_weight)


def reference(query_rows, key_rows, value_rows, document_ids, output_weight):
    group = HEADS // KV
    query_block = 4 * TOK_DEV
    key_span = min(SEQ, MAXDOC + query_block)
    block_count = SEQ // query_block
    scaling = 1.0 / (HD ** 0.5)

    def one_block(block_index):
        query_start = (block_index * query_block).astype(jnp.int32)
        key_start = jnp.clip(query_start + query_block - key_span, 0, SEQ - key_span).astype(jnp.int32)
        queries = lax.dynamic_slice_in_dim(query_rows, query_start, query_block, 0)
        queries = queries.reshape(query_block, KV, group, HD).astype(jnp.float32)
        key_block = lax.dynamic_slice_in_dim(key_rows, key_start, key_span, 0)
        key_block = key_block.reshape(key_span, KV, HD).astype(jnp.float32)
        value_block = lax.dynamic_slice_in_dim(value_rows, key_start, key_span, 0)
        value_block = value_block.reshape(key_span, KV, HD).astype(jnp.float32)
        query_doc = lax.dynamic_slice_in_dim(document_ids, query_start, query_block, 0)
        key_doc = lax.dynamic_slice_in_dim(document_ids, key_start, key_span, 0)
        query_pos = query_start + jnp.arange(query_block, dtype=jnp.int32)
        key_pos = key_start + jnp.arange(key_span, dtype=jnp.int32)
        allowed = (key_doc[None, :] == query_doc[:, None]) & (key_pos[None, :] <= query_pos[:, None])
        scores = jnp.einsum("tkgd,ukd->kgtu", queries, key_block) * scaling
        scores = jnp.where(allowed, scores, -jnp.inf)
        row_max = jnp.max(scores, axis=-1, keepdims=True)
        exponent = jnp.exp(scores - row_max)
        denominator = jnp.sum(exponent, axis=-1)
        rounded = lax.optimization_barrier(exponent.astype(jnp.bfloat16))
        context = jnp.einsum("kgtu,ukd->kgtd", rounded.astype(jnp.float32), value_block)
        context = context / denominator[..., None]
        return context.transpose(2, 0, 1, 3).reshape(query_block, HEADS * HD)

    context = lax.map(one_block, jnp.arange(block_count, dtype=jnp.int32))
    context = context.reshape(SEQ, HEADS * HD).astype(jnp.bfloat16)
    width = HEADS * HD // N_TP
    summed = jnp.zeros((SEQ, D), jnp.float32)
    for group_index in range(N_TP):
        partial_value = jnp.dot(context[:, group_index * width:(group_index + 1) * width],
                          output_weight[group_index * width:(group_index + 1) * width],
                          preferred_element_type=jnp.float32)
        partial_value = lax.optimization_barrier(partial_value.astype(jnp.bfloat16))
        summed = summed + partial_value.astype(jnp.float32)
    return summed.astype(jnp.bfloat16)
```

```python
import functools

import jax
import jax.numpy as jnp
from jax import lax
from jax.experimental import pallas as pl
from jax.experimental.pallas import tpu as pltpu
from jax.sharding import PartitionSpec as P

HEADS = 32
KV = 8
HD = 128
AXES = ("seq", "tp")
LOG2E = 1.4426950408889634
VMEM = pl.BlockSpec(memory_space=pltpu.VMEM)


def routes(seq, tp):
    rows = seq // 2

    def flat(rule):
        pairs = []
        for s in range(seq):
            for t in range(tp):
                s2, t2 = rule(s, t)
                pairs.append((s * tp + t, s2 * tp + t2))
        return pairs

    def by_row(parity):
        def rule(s, t):
            row, col = divmod(s, 2)
            other = row + 1 if row % 2 == parity else row - 1
            if 0 <= other < rows:
                return other * 2 + col, t
            return s, t ^ 1

        return flat(rule)

    return {
        "even": by_row(0),
        "odd": by_row(1),
        "col": flat(lambda s, t: (s ^ 1, t)),
        "core": flat(lambda s, t: (s, t ^ 1)),
    }


def y_route(seq, tp, distance):
    pairs = []
    for s in range(seq):
        for t in range(tp):
            pairs.append((s * tp + t, s * tp + (t + 2 * distance) % tp))
    return pairs


def attend(query, keys, values, bias):
    scores = lax.dot_general(
        query, keys, (((1,), (1,)), ((), ())), preferred_element_type=jnp.float32
    )
    scores = scores * (LOG2E / HD**0.5) + bias
    return scores, jnp.max(scores, axis=-1, keepdims=True)


def early_kernel(kv_local, group, count, *refs):
    q_ref, qdoc_ref, qpos_ref, kdoc_ref = refs[:4]
    blocks = refs[4 : 4 + count]
    acc_ref, ml_ref, bias_ref = refs[4 + count :]
    tokens = q_ref.shape[0]
    allowed = qdoc_ref[...] == kdoc_ref[...]
    key_at = lax.broadcasted_iota(jnp.int32, (tokens, count * tokens), 1)
    allowed = allowed & ((key_at <= qpos_ref[...]) | (key_at >= tokens))
    bias_ref[...] = jnp.where(allowed, 0.0, -jnp.inf)
    lane = lax.broadcasted_iota(jnp.int32, (tokens, 128), 1)
    ml = jnp.zeros((tokens, 128), jnp.float32)
    for h in range(kv_local):
        k_cols = pl.ds(h * HD, HD)
        v_cols = pl.ds((kv_local + h) * HD, HD)
        keys = jnp.concatenate([b[:, k_cols] for b in blocks], axis=0)
        values = jnp.concatenate([b[:, v_cols] for b in blocks], axis=0)
        for g in range(group):
            head = h * group + g
            cols = pl.ds(head * HD, HD)
            scores, top = attend(q_ref[:, cols], keys, values, bias_ref[...])
            weight = jnp.exp2(scores - top)
            total = jnp.sum(weight, axis=-1, keepdims=True)
            acc_ref[:, cols] = jnp.dot(
                weight.astype(jnp.bfloat16), values, preferred_element_type=jnp.float32
            )
            ml = jnp.where(lane == 2 * head, top, ml)
            ml = jnp.where(lane == 2 * head + 1, total, ml)
    ml_ref[...] = ml


def project(context, weight, send_ref, keep_ref, part):
    rows = jnp.dot(context, weight, preferred_element_type=jnp.float32)
    rows = rows.astype(jnp.bfloat16)
    for i in range(rows.shape[0] // (2 * part)):
        at = pl.ds(i * part, part)
        keep_ref[at, :] = rows[2 * i * part : (2 * i + 1) * part]
        send_ref[at, :] = rows[(2 * i + 1) * part : (2 * i + 2) * part]


def late_kernel(kv_local, group, part, *refs):
    q_ref, qdoc_ref, kdoc_ref, block, acc_ref, ml_ref, w_hbm = refs[:7]
    context_ref, send_ref, keep_ref, w_ref, sem = refs[7:]
    tokens = q_ref.shape[0]
    copy = pltpu.make_async_copy(w_hbm.at[:, pl.ds(0, w_ref.shape[1])], w_ref, sem)
    copy.start()
    bias = jnp.where(qdoc_ref[...] == kdoc_ref[...], 0.0, -jnp.inf)
    ml = ml_ref[...]
    for h in range(kv_local):
        keys = block[:, pl.ds(h * HD, HD)]
        values = block[:, pl.ds((kv_local + h) * HD, HD)]
        for g in range(group):
            head = h * group + g
            cols = pl.ds(head * HD, HD)
            scores, top = attend(q_ref[:, cols], keys, values, bias)
            old = ml[:, 2 * head : 2 * head + 1]
            new = jnp.maximum(old, top)
            weight = jnp.exp2(scores - new)
            rescale = jnp.exp2(old - new)
            total = ml[:, 2 * head + 1 : 2 * head + 2] * rescale
            total = total + jnp.sum(weight, axis=-1, keepdims=True)
            added = jnp.dot(
                weight.astype(jnp.bfloat16), values, preferred_element_type=jnp.float32
            )
            context = (acc_ref[:, cols] * rescale + added) / total
            context_ref[:, cols] = context.astype(jnp.bfloat16)
    copy.wait()
    project(context_ref[...], w_ref[...], send_ref, keep_ref, part)


def project_kernel(part, context_ref, w_ref, send_ref, keep_ref):
    project(context_ref[...], w_ref[...], send_ref, keep_ref, part)


def project_call(context, weight, start, width, part, block):
    tokens, depth = context.shape
    half = tokens // 2
    out = jax.ShapeDtypeStruct((half, width), jnp.bfloat16)
    out_spec = pl.BlockSpec((half, block), lambda i: (0, i))
    return pl.pallas_call(
        functools.partial(project_kernel, part),
        out_shape=(out, out),
        grid=(width // block,),
        in_specs=[
            pl.BlockSpec((tokens, depth), lambda i: (0, 0)),
            pl.BlockSpec((depth, block), lambda i: (0, start // block + i)),
        ],
        out_specs=(out_spec, out_spec),
        cost_estimate=pl.CostEstimate(
            flops=2 * tokens * depth * width,
            transcendentals=0,
            bytes_accessed=2 * depth * width,
        ),
        name="project_rest",
    )(context, weight)


def per_device(query_rows, key_rows, value_rows, document_ids, output_weight):
    tokens = query_rows.shape[0]
    kv_local = key_rows.shape[1] // HD
    group = HEADS // KV
    width = query_rows.shape[1]
    model = output_weight.shape[1]
    seq, tp = lax.axis_size("seq"), lax.axis_size("tp")
    part = tokens // tp
    chips = tp // 2
    reach = min(12, seq // 2)
    depth = (reach + 1) // 2
    route = routes(seq, tp)
    me, rank = lax.axis_index("seq"), lax.axis_index("tp")
    row, col = me // 2, me % 2
    odd_row = row % 2 == 1

    def send(x, name):
        return lax.ppermute(x, AXES, route[name])

    own = jnp.concatenate([key_rows, value_rows], axis=1)
    even, odd = send(own, "even"), send(own, "odd")
    mine, theirs = [own], [send(own, "col")]
    for distance in range(1, depth + 1):
        mine.append(jnp.where(odd_row, even, odd))
        if distance < depth:
            even, odd = send(odd, "even"), send(even, "odd")
        theirs.append(send(mine[-1], "col"))

    groups = []
    for distance in range(1, chips + 1):
        base = (rank // 2 + distance) % chips * 2
        groups += [(base + rank % 2) * part, (base + 1 - rank % 2) * part]
    queries = jnp.concatenate(
        [lax.dynamic_slice_in_dim(query_rows, g, part, 0) for g in groups], axis=0
    )
    spot = jnp.arange(part, dtype=jnp.int32)
    qpos = jnp.concatenate([g + spot for g in groups])
    first = me * tokens
    own_doc = lax.dynamic_slice_in_dim(document_ids, first, tokens, 0)
    qdoc = jnp.concatenate(
        [lax.dynamic_slice_in_dim(own_doc, g, part, 0) for g in groups]
    )
    qpos, qdoc = qpos[:, None], qdoc[:, None]

    def doc_of(block):
        ids = lax.dynamic_slice_in_dim(
            document_ids, jnp.maximum(block, 0) * tokens, tokens, 0
        )
        return jnp.where((block >= 0) & (block <= me), ids, -1)

    blocks, docs = [mine[0]], [doc_of(me)]
    for distance in range(depth + 1):
        if distance:
            blocks.append(mine[distance])
            docs.append(doc_of(me - 2 * distance))
        blocks.append(theirs[distance])
        docs.append(doc_of((row - distance) * 2 + 1 - col))
    last_block, last_doc = blocks.pop(), docs.pop()[None, :]
    count = len(blocks)
    docs = jnp.concatenate(docs)[None, :]

    acc, ml = pl.pallas_call(
        functools.partial(early_kernel, kv_local, group, count),
        out_shape=(
            jax.ShapeDtypeStruct((tokens, width), jnp.float32),
            jax.ShapeDtypeStruct((tokens, 128), jnp.float32),
        ),
        in_specs=[VMEM] * (4 + count),
        out_specs=(VMEM, VMEM),
        scratch_shapes=[pltpu.VMEM((tokens, count * tokens), jnp.float32)],
        cost_estimate=pl.CostEstimate(
            flops=4 * tokens * tokens * count * width,
            transcendentals=tokens * tokens * count * width // HD,
            bytes_accessed=4 * tokens * width,
        ),
        name="attend_early",
    )(queries, qdoc, qpos, docs, *blocks)

    cuts = [model * 3 // 16, model // 2, model]
    half = tokens // 2
    out = jax.ShapeDtypeStruct((half, cuts[0]), jnp.bfloat16)
    context, sent, kept = pl.pallas_call(
        functools.partial(late_kernel, kv_local, group, part),
        out_shape=(jax.ShapeDtypeStruct((tokens, width), jnp.bfloat16), out, out),
        in_specs=[VMEM] * 6 + [pl.BlockSpec(memory_space=pl.ANY)],
        out_specs=(VMEM, VMEM, VMEM),
        scratch_shapes=[
            pltpu.VMEM((width, cuts[0]), jnp.bfloat16),
            pltpu.SemaphoreType.DMA,
        ],
        cost_estimate=pl.CostEstimate(
            flops=4 * tokens * tokens * width + 2 * tokens * width * cuts[0],
            transcendentals=tokens * tokens * width // HD,
            bytes_accessed=4 * tokens * width + 2 * width * cuts[0],
        ),
        name="attend_late",
    )(queries, qdoc, last_doc, last_block, acc, ml, output_weight)

    pieces = []
    remote = (chips - 1) * part
    for i, stop in enumerate(cuts):
        if i:
            start = cuts[i - 1]
            sent, kept = project_call(
                context, output_weight, start, stop - start, part, 512
            )
        received = send(sent, "core")
        total = kept.astype(jnp.float32) + received.astype(jnp.float32)
        moved = total[:remote].astype(jnp.bfloat16)
        piece = total[remote:]
        for distance in range(1, chips):
            at = (distance - 1) * part
            arrived = lax.ppermute(
                moved[at : at + part], AXES, y_route(seq, tp, distance)
            )
            piece = piece + arrived.astype(jnp.float32)
        pieces.append(piece.astype(jnp.bfloat16))
    return jnp.concatenate(pieces, axis=1)


def solution(mesh):
    in_specs = (P("seq", "tp"), P("seq", "tp"), P("seq", "tp"), P(), P("tp", None))
    out_specs = P(("seq", "tp"), None)
    return jax.shard_map(
        per_device, mesh=mesh, in_specs=in_specs, out_specs=out_specs, check_vma=False
    )
```

```python
import functools

import jax
import jax.numpy as jnp
from jax import lax
from jax.experimental import pallas as pl
from jax.experimental.pallas import tpu as pltpu
from jax.sharding import PartitionSpec as P


HEADS = 32
KV = 8
HD = 128
AXES = ("seq", "tp")
LOG2E = 1.4426950408889634
SCALE = LOG2E / HD**0.5
VMEM = pl.BlockSpec(memory_space=pltpu.VMEM)
ANY = pl.BlockSpec(memory_space=pl.ANY)
MIB = 1 << 20


def routes(seq, tp):
    rows = seq // 2

    def flat(rule):
        pairs = []
        for s in range(seq):
            for t in range(tp):
                s2, t2 = rule(s, t)
                pairs.append((s * tp + t, s2 * tp + t2))
        return pairs

    def by_row(parity):
        def rule(s, t):
            row, col = divmod(s, 2)
            other = row + 1 if row % 2 == parity else row - 1
            if 0 <= other < rows:
                return other * 2 + col, t
            return s, t ^ 1

        return flat(rule)

    return {
        "even": by_row(0),
        "odd": by_row(1),
        "col": flat(lambda s, t: (s ^ 1, t)),
        "core": flat(lambda s, t: (s, t ^ 1)),
    }


def y_route(seq, tp, distance):
    pairs = []
    for s in range(seq):
        for t in range(tp):
            pairs.append((s * tp + t, s * tp + (t + 2 * distance) % tp))
    return pairs


def join_kernel(k_ref, v_ref, out_ref, sems):
    width = k_ref.shape[1]
    copies = [
        pltpu.make_async_copy(k_ref, out_ref.at[:, pl.ds(0, width)], sems.at[0]),
        pltpu.make_async_copy(v_ref, out_ref.at[:, pl.ds(width, width)], sems.at[1]),
    ]
    for copy in copies:
        copy.start()
    for copy in copies:
        copy.wait()


def query_doc(docs_t_ref, me):
    docs = docs_t_ref[...]
    lane = lax.broadcasted_iota(jnp.int32, docs.shape, 1)
    return jnp.sum(jnp.where(lane == me, docs, 0.0), axis=1, keepdims=True)


def key_doc(docs_ref, block, me):
    row = docs_ref[pl.ds(jnp.maximum(block, 0), 1), :]
    return jnp.where((block >= 0) & (block <= me), row, -1.0)


def stack(q_ref, h, group):
    return jnp.concatenate(
        [q_ref[:, pl.ds((h * group + g) * HD, HD)] for g in range(group)], axis=0
    )


def scores_of(queries, keys):
    return lax.dot_general(
        queries, keys, (((1,), (1,)), ((), ())), preferred_element_type=jnp.float32
    )


def early_kernel(kv_local, group, count, step, *refs):
    q_ref, docs_ref, docs_t_ref = refs[:3]
    blocks = refs[3 : 3 + count]
    w_hbm = refs[3 + count]
    acc_ref, top_ref, sum_ref, w_ref = refs[4 + count : 8 + count]
    bias_ref, s_ref, p_ref, sem = refs[8 + count :]
    copy = pltpu.make_async_copy(w_hbm, w_ref, sem)
    copy.start()
    tokens = q_ref.shape[0]
    stacked = group * tokens
    me = lax.axis_index("seq")
    row, col = me // 2, me % 2
    docs = []
    for i in range(count):
        block = me - i if i % 2 == 0 else (row - i // 2) * 2 + 1 - col
        docs.append(key_doc(docs_ref, block, me))
    allowed = query_doc(docs_t_ref, me) == jnp.concatenate(docs, axis=1)
    key_at = lax.broadcasted_iota(jnp.int32, (tokens, count * tokens), 1)
    query_at = lax.broadcasted_iota(jnp.int32, (tokens, count * tokens), 0)
    allowed = allowed & ((key_at <= query_at) | (key_at >= tokens))
    bias_ref[...] = jnp.where(allowed, 0.0, -jnp.inf)
    for h in range(kv_local):
        keys = jnp.concatenate([b[:, pl.ds(h * HD, HD)] for b in blocks], axis=0)
        s_ref[...] = scores_of(stack(q_ref, h, group), keys)
        for r in range(0, stacked, step):
            at = pl.ds(r, step)
            into = pl.ds(h * stacked + r, step)
            scores = s_ref[at, :] * SCALE + bias_ref[pl.ds(r % tokens, step), :]
            top = jnp.max(scores, axis=-1, keepdims=True)
            weight = jnp.exp2(scores - top)
            total = jnp.sum(weight, axis=-1, keepdims=True)
            p_ref[at, :] = weight.astype(jnp.bfloat16)
            top_ref[into, :] = jnp.broadcast_to(top, (step, HD))
            sum_ref[into, :] = jnp.broadcast_to(total, (step, HD))
        cols = pl.ds((kv_local + h) * HD, HD)
        values = jnp.concatenate([b[:, cols] for b in blocks], axis=0)
        acc_ref[pl.ds(h * stacked, stacked), :] = jnp.dot(
            p_ref[...], values, preferred_element_type=jnp.float32
        )
    copy.wait()


def project(context_ref, w_ref, start, width, send_ref, keep_ref, part):
    step = 512
    for c in range(0, width, step):
        at = pl.ds(c, step)
        rows = jnp.dot(
            context_ref[...],
            w_ref[:, pl.ds(start + c, step)],
            preferred_element_type=jnp.float32,
        ).astype(jnp.bfloat16)
        for i in range(rows.shape[0] // (2 * part)):
            into = pl.ds(i * part, part)
            keep_ref[into, at] = rows[2 * i * part : (2 * i + 1) * part]
            send_ref[into, at] = rows[(2 * i + 1) * part : (2 * i + 2) * part]


def late_kernel(kv_local, group, part, depth, *refs):
    q_ref, docs_ref, docs_t_ref, block, acc_ref, top_ref, sum_ref, w_ref = refs[:8]
    out_ref, send_ref, keep_ref, context_ref = refs[8:]
    tokens = q_ref.shape[0]
    stacked = group * tokens
    me, rank = lax.axis_index("seq"), lax.axis_index("tp")
    chips = lax.axis_size("tp") // 2
    far = (me // 2 - depth) * 2 + 1 - me % 2
    bias = jnp.where(
        query_doc(docs_t_ref, me) == key_doc(docs_ref, far, me), 0.0, -jnp.inf
    )
    for h in range(kv_local):
        keys = block[:, pl.ds(h * HD, HD)]
        values = block[:, pl.ds((kv_local + h) * HD, HD)]
        scores = scores_of(stack(q_ref, h, group), keys)
        scores = scores * SCALE + jnp.concatenate([bias] * group, axis=0)
        at = pl.ds(h * stacked, stacked)
        old = top_ref[at, :]
        new = jnp.maximum(old[:, :1], jnp.max(scores, axis=-1, keepdims=True))
        weight = jnp.exp2(scores - new)
        rescale = jnp.exp2(old - new)
        total = sum_ref[at, :] * rescale + jnp.sum(weight, axis=-1, keepdims=True)
        added = jnp.dot(
            weight.astype(jnp.bfloat16), values, preferred_element_type=jnp.float32
        )
        context = (acc_ref[at, :] * rescale + added) / total
        context = context.astype(jnp.bfloat16)
        for g in range(group):
            cols = pl.ds((h * group + g) * HD, HD)
            context_ref[:, cols] = context[g * tokens : (g + 1) * tokens]
    at = 0
    for distance in range(1, chips + 1):
        base = lax.rem(rank // 2 + distance, chips) * 2
        for core in (rank % 2, 1 - rank % 2):
            first = pl.multiple_of((base + core) * part, 8)
            out_ref[pl.ds(at, part), :] = context_ref[pl.ds(first, part), :]
            at += part
    project(out_ref, w_ref, 0, send_ref.shape[1], send_ref, keep_ref, part)


def project_kernel(part, start, context_ref, w_ref, send_ref, keep_ref):
    width = send_ref.shape[1]
    project(context_ref, w_ref, start, width, send_ref, keep_ref, part)


def project_call(context, weight, start, width, part):
    tokens, depth = context.shape
    out = jax.ShapeDtypeStruct((tokens // 2, width), jnp.bfloat16)
    return pl.pallas_call(
        functools.partial(project_kernel, part, start),
        out_shape=(out, out),
        in_specs=[VMEM, VMEM],
        out_specs=(VMEM, VMEM),
        cost_estimate=pl.CostEstimate(
            flops=2 * tokens * depth * width,
            transcendentals=0,
            bytes_accessed=2 * depth * width,
        ),
        compiler_params=pltpu.CompilerParams(vmem_limit_bytes=8 * MIB),
        name="project_rest",
    )(context, weight)


def layer(query_rows, key_rows, value_rows, document_ids, output_weight):
    tokens = query_rows.shape[0]
    kv_local = key_rows.shape[1] // HD
    group = HEADS // KV
    width = query_rows.shape[1]
    model = output_weight.shape[1]
    seq, tp = lax.axis_size("seq"), lax.axis_size("tp")
    part = tokens // tp
    chips = tp // 2
    reach = min(12, seq // 2)
    depth = (reach + 1) // 2
    route = routes(seq, tp)
    odd_row = (lax.axis_index("seq") // 2) % 2 == 1

    def send(x, name):
        return lax.ppermute(x, AXES, route[name])

    own = pl.pallas_call(
        join_kernel,
        out_shape=jax.ShapeDtypeStruct((tokens, 2 * kv_local * HD), jnp.bfloat16),
        in_specs=[ANY, ANY],
        out_specs=VMEM,
        scratch_shapes=[pltpu.SemaphoreType.DMA((2,))],
        compiler_params=pltpu.CompilerParams(vmem_limit_bytes=2 * MIB),
        name="join",
    )(key_rows, value_rows)
    docs = document_ids.astype(jnp.float32).reshape(seq, tokens)
    docs_t = docs.T
    even, odd = send(own, "even"), send(own, "odd")
    blocks = [own, send(own, "col")]
    even, odd, docs, docs_t = lax.optimization_barrier((even, odd, docs, docs_t))
    for distance in range(1, depth + 1):
        blocks.append(jnp.where(odd_row, even, odd))
        if distance < depth:
            even, odd = send(odd, "even"), send(even, "odd")
        blocks.append(send(blocks[-1], "col"))
    last_block = blocks.pop()
    count = len(blocks)

    stacked = group * tokens
    state = jax.ShapeDtypeStruct((kv_local * stacked, HD), jnp.float32)
    acc, top, total, weight = pl.pallas_call(
        functools.partial(early_kernel, kv_local, group, count, 32),
        out_shape=(
            state,
            state,
            state,
            pltpu.VMEM(output_weight.shape, output_weight.dtype),
        ),
        in_specs=[VMEM] * (3 + count) + [ANY],
        out_specs=(VMEM,) * 4,
        scratch_shapes=[
            pltpu.VMEM((tokens, count * tokens), jnp.float32),
            pltpu.VMEM((stacked, count * tokens), jnp.float32),
            pltpu.VMEM((stacked, count * tokens), jnp.bfloat16),
            pltpu.SemaphoreType.DMA,
        ],
        cost_estimate=pl.CostEstimate(
            flops=4 * tokens * tokens * count * width,
            transcendentals=tokens * tokens * count * width // HD,
            bytes_accessed=2 * width * model,
        ),
        compiler_params=pltpu.CompilerParams(vmem_limit_bytes=24 * MIB),
        name="attend_early",
    )(query_rows, docs, docs_t, *blocks, output_weight)

    cuts = [model * 3 // 16, model // 2, model]
    out = jax.ShapeDtypeStruct((tokens // 2, cuts[0]), jnp.bfloat16)
    context, sent, kept = pl.pallas_call(
        functools.partial(late_kernel, kv_local, group, part, depth),
        out_shape=(jax.ShapeDtypeStruct((tokens, width), jnp.bfloat16), out, out),
        in_specs=[VMEM] * 8,
        out_specs=(VMEM, VMEM, VMEM),
        scratch_shapes=[pltpu.VMEM((tokens, width), jnp.bfloat16)],
        cost_estimate=pl.CostEstimate(
            flops=4 * tokens * tokens * width + 2 * tokens * width * cuts[0],
            transcendentals=tokens * tokens * width // HD,
            bytes_accessed=4 * tokens * width + 2 * width * cuts[0],
        ),
        compiler_params=pltpu.CompilerParams(vmem_limit_bytes=16 * MIB),
        name="attend_late",
    )(query_rows, docs, docs_t, last_block, acc, top, total, weight)

    pieces = []
    remote = (chips - 1) * part
    for i, stop in enumerate(cuts):
        if i:
            start = cuts[i - 1]
            sent, kept = project_call(context, weight, start, stop - start, part)
        received = send(sent, "core")
        moved = (
            kept[:remote].astype(jnp.float32) + received[:remote].astype(jnp.float32)
        ).astype(jnp.bfloat16)
        context, moved = lax.optimization_barrier((context, moved))
        piece = kept[remote:].astype(jnp.float32) + received[remote:].astype(
            jnp.float32
        )
        for distance in range(1, chips):
            at = (distance - 1) * part
            arrived = lax.ppermute(
                moved[at : at + part], AXES, y_route(seq, tp, distance)
            )
            piece = piece + arrived.astype(jnp.float32)
        pieces.append(piece.astype(jnp.bfloat16))
    return jnp.concatenate(pieces, axis=1)


def solution(mesh):
    in_specs = (P("seq", "tp"), P("seq", "tp"), P("seq", "tp"), P(), P("tp", None))
    out_specs = P(("seq", "tp"), None)
    return jax.shard_map(
        layer, mesh=mesh, in_specs=in_specs, out_specs=out_specs, check_vma=False
    )
```

```python
import functools

import jax
import jax.numpy as jnp
from jax import lax
from jax.experimental import pallas as pl
from jax.experimental.pallas import tpu as pltpu
from jax.sharding import PartitionSpec as P


HEADS = 32
KV = 8
HD = 128
AXES = ("seq", "tp")
LOG2E = 1.4426950408889634
SCALE = LOG2E / HD**0.5
VMEM = pl.BlockSpec(memory_space=pltpu.VMEM)
ANY = pl.BlockSpec(memory_space=pl.ANY)
MIB = 1 << 20


def routes(seq, tp):
    rows = seq // 2

    def flat(rule):
        pairs = []
        for s in range(seq):
            for t in range(tp):
                s2, t2 = rule(s, t)
                pairs.append((s * tp + t, s2 * tp + t2))
        return pairs

    def by_row(parity):
        def rule(s, t):
            row, col = divmod(s, 2)
            other = row + 1 if row % 2 == parity else row - 1
            if 0 <= other < rows:
                return other * 2 + col, t
            return s, t ^ 1

        return flat(rule)

    return {
        "even": by_row(0),
        "odd": by_row(1),
        "col": flat(lambda s, t: (s ^ 1, t)),
        "core": flat(lambda s, t: (s, t ^ 1)),
    }


def y_route(seq, tp, distance):
    pairs = []
    for s in range(seq):
        for t in range(tp):
            pairs.append((s * tp + t, s * tp + (t + 2 * distance) % tp))
    return pairs


def join_kernel(k_ref, v_ref, out_ref, sems):
    width = k_ref.shape[1]
    copies = [
        pltpu.make_async_copy(k_ref, out_ref.at[:, pl.ds(0, width)], sems.at[0]),
        pltpu.make_async_copy(v_ref, out_ref.at[:, pl.ds(width, width)], sems.at[1]),
    ]
    for copy in copies:
        copy.start()
    for copy in copies:
        copy.wait()


def load_kernel(start, w_hbm, out_ref, sem):
    width = out_ref.shape[1]
    copy = pltpu.make_async_copy(w_hbm.at[:, pl.ds(start, width)], out_ref, sem)
    copy.start()
    copy.wait()


def load_call(weight, start, stop):
    shape = (weight.shape[0], stop - start)
    return pl.pallas_call(
        functools.partial(load_kernel, start),
        out_shape=pltpu.VMEM(shape, weight.dtype),
        in_specs=[ANY],
        out_specs=VMEM,
        scratch_shapes=[pltpu.SemaphoreType.DMA],
        cost_estimate=pl.CostEstimate(
            flops=0, transcendentals=0, bytes_accessed=2 * shape[0] * shape[1]
        ),
        compiler_params=pltpu.CompilerParams(vmem_limit_bytes=MIB),
        name="load",
    )(weight)


def in_hbm(x):
    return pltpu.with_memory_space_constraint(x, pltpu.HBM)


def query_doc(docs_t_ref, me):
    docs = docs_t_ref[...]
    lane = lax.broadcasted_iota(jnp.int32, docs.shape, 1)
    return jnp.sum(jnp.where(lane == me, docs, 0.0), axis=1, keepdims=True)


def key_doc(docs_ref, block, me):
    row = docs_ref[pl.ds(jnp.maximum(block, 0), 1), :]
    return jnp.where((block >= 0) & (block <= me), row, -1.0)


def stack(q_ref, h, group):
    return jnp.concatenate(
        [q_ref[:, pl.ds((h * group + g) * HD, HD)] for g in range(group)], axis=0
    )


def scores_of(queries, keys):
    return lax.dot_general(
        queries, keys, (((1,), (1,)), ((), ())), preferred_element_type=jnp.float32
    )


def early_kernel(kv_local, group, count, step, *refs):
    q_ref, docs_ref, docs_t_ref = refs[:3]
    blocks = refs[3 : 3 + count]
    acc_ref, top_ref, sum_ref = refs[3 + count : 6 + count]
    bias_ref, s_ref, p_ref = refs[6 + count :]
    tokens = q_ref.shape[0]
    stacked = group * tokens
    me = lax.axis_index("seq")
    row, col = me // 2, me % 2
    docs = []
    for i in range(count):
        block = me - i if i % 2 == 0 else (row - i // 2) * 2 + 1 - col
        docs.append(key_doc(docs_ref, block, me))
    allowed = query_doc(docs_t_ref, me) == jnp.concatenate(docs, axis=1)
    key_at = lax.broadcasted_iota(jnp.int32, (tokens, count * tokens), 1)
    query_at = lax.broadcasted_iota(jnp.int32, (tokens, count * tokens), 0)
    allowed = allowed & ((key_at <= query_at) | (key_at >= tokens))
    bias_ref[...] = jnp.where(allowed, 0.0, -jnp.inf)
    for h in range(kv_local):
        keys = jnp.concatenate([b[:, pl.ds(h * HD, HD)] for b in blocks], axis=0)
        s_ref[...] = scores_of(stack(q_ref, h, group), keys)
        for r in range(0, stacked, step):
            at = pl.ds(r, step)
            into = pl.ds(h * stacked + r, step)
            scores = s_ref[at, :] * SCALE + bias_ref[pl.ds(r % tokens, step), :]
            top = jnp.max(scores, axis=-1, keepdims=True)
            weight = jnp.exp2(scores - top)
            total = jnp.sum(weight, axis=-1, keepdims=True)
            p_ref[at, :] = weight.astype(jnp.bfloat16)
            top_ref[into, :] = jnp.broadcast_to(top, (step, HD))
            sum_ref[into, :] = jnp.broadcast_to(total, (step, HD))
        cols = pl.ds((kv_local + h) * HD, HD)
        values = jnp.concatenate([b[:, cols] for b in blocks], axis=0)
        acc_ref[pl.ds(h * stacked, stacked), :] = jnp.dot(
            p_ref[...], values, preferred_element_type=jnp.float32
        )


def project(context_ref, w_ref, start, width, send_ref, keep_ref, part):
    step = 256
    for c in range(0, width, step):
        at = pl.ds(c, step)
        rows = jnp.dot(
            context_ref[...],
            w_ref[:, pl.ds(start + c, step)],
            preferred_element_type=jnp.float32,
        ).astype(jnp.bfloat16)
        for i in range(rows.shape[0] // (2 * part)):
            into = pl.ds(i * part, part)
            keep_ref[into, at] = rows[2 * i * part : (2 * i + 1) * part]
            send_ref[into, at] = rows[(2 * i + 1) * part : (2 * i + 2) * part]


def late_kernel(kv_local, group, part, depth, *refs):
    q_ref, docs_ref, docs_t_ref, block, acc_ref, top_ref, sum_ref, w_ref = refs[:8]
    out_ref, send_ref, keep_ref, context_ref = refs[8:]
    tokens = q_ref.shape[0]
    stacked = group * tokens
    me, rank = lax.axis_index("seq"), lax.axis_index("tp")
    chips = lax.axis_size("tp") // 2
    far = (me // 2 - depth) * 2 + 1 - me % 2
    bias = jnp.where(
        query_doc(docs_t_ref, me) == key_doc(docs_ref, far, me), 0.0, -jnp.inf
    )
    for h in range(kv_local):
        keys = block[:, pl.ds(h * HD, HD)]
        values = block[:, pl.ds((kv_local + h) * HD, HD)]
        scores = scores_of(stack(q_ref, h, group), keys)
        scores = scores * SCALE + jnp.concatenate([bias] * group, axis=0)
        at = pl.ds(h * stacked, stacked)
        old = top_ref[at, :]
        new = jnp.maximum(old[:, :1], jnp.max(scores, axis=-1, keepdims=True))
        weight = jnp.exp2(scores - new)
        rescale = jnp.exp2(old - new)
        total = sum_ref[at, :] * rescale + jnp.sum(weight, axis=-1, keepdims=True)
        added = jnp.dot(
            weight.astype(jnp.bfloat16), values, preferred_element_type=jnp.float32
        )
        context = (acc_ref[at, :] * rescale + added) / total
        context = context.astype(jnp.bfloat16)
        for g in range(group):
            cols = pl.ds((h * group + g) * HD, HD)
            context_ref[:, cols] = context[g * tokens : (g + 1) * tokens]
    at = 0
    for distance in range(1, chips + 1):
        base = lax.rem(rank // 2 + distance, chips) * 2
        for core in (rank % 2, 1 - rank % 2):
            first = pl.multiple_of((base + core) * part, 8)
            out_ref[pl.ds(at, part), :] = context_ref[pl.ds(first, part), :]
            at += part
    project(out_ref, w_ref, 0, send_ref.shape[1], send_ref, keep_ref, part)


def project_kernel(part, start, context_ref, w_ref, send_ref, keep_ref):
    width = send_ref.shape[1]
    project(context_ref, w_ref, start, width, send_ref, keep_ref, part)


def project_call(context, weight, start, width, part):
    tokens, depth = context.shape
    out = jax.ShapeDtypeStruct((tokens // 2, width), jnp.bfloat16)
    return pl.pallas_call(
        functools.partial(project_kernel, part, start),
        out_shape=(out, out),
        in_specs=[VMEM, VMEM],
        out_specs=(VMEM, VMEM),
        cost_estimate=pl.CostEstimate(
            flops=2 * tokens * depth * width,
            transcendentals=0,
            bytes_accessed=2 * depth * width,
        ),
        compiler_params=pltpu.CompilerParams(vmem_limit_bytes=8 * MIB),
        name="project_rest",
    )(context, weight)


def layer(query_rows, key_rows, value_rows, document_ids, output_weight):
    tokens = query_rows.shape[0]
    kv_local = key_rows.shape[1] // HD
    group = HEADS // KV
    width = query_rows.shape[1]
    model = output_weight.shape[1]
    seq, tp = lax.axis_size("seq"), lax.axis_size("tp")
    part = tokens // tp
    chips = tp // 2
    reach = min(12, seq // 2)
    depth = (reach + 1) // 2
    route = routes(seq, tp)
    odd_row = (lax.axis_index("seq") // 2) % 2 == 1

    def send(x, name):
        return lax.ppermute(x, AXES, route[name])

    own = pl.pallas_call(
        join_kernel,
        out_shape=pltpu.VMEM((tokens, 2 * kv_local * HD), jnp.bfloat16),
        in_specs=[ANY, ANY],
        out_specs=VMEM,
        scratch_shapes=[pltpu.SemaphoreType.DMA((2,))],
        compiler_params=pltpu.CompilerParams(vmem_limit_bytes=2 * MIB),
        name="join",
    )(in_hbm(key_rows), in_hbm(value_rows))
    docs = document_ids.astype(jnp.float32).reshape(seq, tokens)
    docs_t = docs.T
    cuts = [model * 7 // 32, model * 17 // 32, model]
    weight = in_hbm(output_weight)
    near_weight = load_call(weight, 0, cuts[1])
    far_weight = load_call(weight, cuts[1], model)
    even, odd = send(own, "even"), send(own, "odd")
    blocks = [own, send(own, "col")]
    even, odd, docs, docs_t = lax.optimization_barrier((even, odd, docs, docs_t))
    for distance in range(1, depth + 1):
        blocks.append(jnp.where(odd_row, even, odd))
        if distance < depth:
            even, odd = (send(odd, "even"), send(even, "odd"))
        blocks.append(send(blocks[-1], "col"))
    last_block = blocks.pop()
    count = len(blocks)

    stacked = group * tokens
    state = jax.ShapeDtypeStruct((kv_local * stacked, HD), jnp.float32)
    acc, top, total = pl.pallas_call(
        functools.partial(early_kernel, kv_local, group, count, 32),
        out_shape=(state, state, state),
        in_specs=[VMEM] * (3 + count),
        out_specs=(VMEM,) * 3,
        scratch_shapes=[
            pltpu.VMEM((tokens, count * tokens), jnp.float32),
            pltpu.VMEM((stacked, count * tokens), jnp.float32),
            pltpu.VMEM((stacked, count * tokens), jnp.bfloat16),
        ],
        cost_estimate=pl.CostEstimate(
            flops=4 * tokens * tokens * count * width,
            transcendentals=tokens * tokens * count * width // HD,
            bytes_accessed=4 * tokens * width,
        ),
        compiler_params=pltpu.CompilerParams(vmem_limit_bytes=24 * MIB),
        name="attend_early",
    )(query_rows, docs, docs_t, *blocks)

    out = jax.ShapeDtypeStruct((tokens // 2, cuts[0]), jnp.bfloat16)
    context, sent, kept = pl.pallas_call(
        functools.partial(late_kernel, kv_local, group, part, depth),
        out_shape=(jax.ShapeDtypeStruct((tokens, width), jnp.bfloat16), out, out),
        in_specs=[VMEM] * 8,
        out_specs=(VMEM, VMEM, VMEM),
        scratch_shapes=[pltpu.VMEM((tokens, width), jnp.bfloat16)],
        cost_estimate=pl.CostEstimate(
            flops=4 * tokens * tokens * width + 2 * tokens * width * cuts[0],
            transcendentals=tokens * tokens * width // HD,
            bytes_accessed=4 * tokens * width + 2 * width * cuts[0],
        ),
        compiler_params=pltpu.CompilerParams(vmem_limit_bytes=16 * MIB),
        name="attend_late",
    )(query_rows, docs, docs_t, last_block, acc, top, total, near_weight)

    pieces = []
    remote = (chips - 1) * part
    for i, stop in enumerate(cuts):
        if i:
            from_weight = near_weight if i == 1 else far_weight
            start = cuts[0] if i == 1 else 0
            sent, kept = project_call(
                context, from_weight, start, stop - cuts[i - 1], part
            )
        received = send(sent, "core")
        moved = (
            kept[:remote].astype(jnp.float32) + received[:remote].astype(jnp.float32)
        ).astype(jnp.bfloat16)
        piece = kept[remote:].astype(jnp.float32) + received[remote:].astype(
            jnp.float32
        )
        for distance in range(1, chips):
            at = (distance - 1) * part
            arrived = lax.ppermute(
                moved[at : at + part], AXES, y_route(seq, tp, distance)
            )
            piece = piece + arrived.astype(jnp.float32)
        pieces.append(piece.astype(jnp.bfloat16))
    return jnp.concatenate(pieces, axis=1)


def solution(mesh):
    in_specs = (P("seq", "tp"), P("seq", "tp"), P("seq", "tp"), P(), P("tp", None))
    out_specs = P(("seq", "tp"), None)
    return jax.shard_map(
        layer, mesh=mesh, in_specs=in_specs, out_specs=out_specs, check_vma=False
    )
```

```python
import functools

import jax
import jax.numpy as jnp
from jax import lax
from jax.experimental import pallas as pl
from jax.experimental.pallas import tpu as pltpu
from jax.sharding import PartitionSpec as P


HEADS = 32
KV = 8
HD = 128
AXES = ("seq", "tp")
LOG2E = 1.4426950408889634
SCALE = LOG2E / HD**0.5
VMEM = pl.BlockSpec(memory_space=pltpu.VMEM)
ANY = pl.BlockSpec(memory_space=pl.ANY)
MIB = 1 << 20


def routes(seq, tp, depth):
    rows = seq // 2

    def flat(rule):
        pairs = []
        for s in range(seq):
            for t in range(tp):
                s2, t2 = rule(s, t)
                pairs.append((s * tp + t, s2 * tp + t2))
        return pairs

    def by_row(parity, step):
        def rule(s, t):
            row, col = divmod(s, 2)
            other = row + 1 if row % 2 == parity else row - 1
            if step - 1 <= min(row, other) and max(row, other) < rows:
                return other * 2 + col, t
            return s, t ^ 1

        return flat(rule)

    def by_col(step):
        return flat(lambda s, t: (s ^ 1, t) if s // 2 >= step else (s, t ^ 1))

    table = {("core", i): flat(lambda s, t: (s, t ^ 1)) for i in range(3)}
    for step in range(depth + 1):
        table["col", step] = by_col(step)
        table["even", step] = by_row(0, step)
        table["odd", step] = by_row(1, step)
    return table


def y_route(seq, tp, distance):
    pairs = []
    for s in range(seq):
        for t in range(tp):
            pairs.append((s * tp + t, s * tp + (t + 2 * distance) % tp))
    return pairs


def join_kernel(k_ref, v_ref, out_ref, sems):
    width = k_ref.shape[1]
    copies = [
        pltpu.make_async_copy(k_ref, out_ref.at[:, pl.ds(0, width)], sems.at[0]),
        pltpu.make_async_copy(v_ref, out_ref.at[:, pl.ds(width, width)], sems.at[1]),
    ]
    for copy in copies:
        copy.start()
    for copy in copies:
        copy.wait()


def load_kernel(start, w_hbm, out_ref, sem):
    width = out_ref.shape[1]
    copy = pltpu.make_async_copy(w_hbm.at[:, pl.ds(start, width)], out_ref, sem)
    copy.start()
    copy.wait()


def load_call(weight, start, stop):
    shape = (weight.shape[0], stop - start)
    return pl.pallas_call(
        functools.partial(load_kernel, start),
        out_shape=pltpu.VMEM(shape, weight.dtype),
        in_specs=[ANY],
        out_specs=VMEM,
        scratch_shapes=[pltpu.SemaphoreType.DMA],
        cost_estimate=pl.CostEstimate(
            flops=0, transcendentals=0, bytes_accessed=2 * shape[0] * shape[1]
        ),
        compiler_params=pltpu.CompilerParams(vmem_limit_bytes=MIB),
        name="load",
    )(weight)


def in_hbm(x):
    return pltpu.with_memory_space_constraint(x, pltpu.HBM)


def query_doc(docs_t_ref, me):
    docs = docs_t_ref[...]
    lane = lax.broadcasted_iota(jnp.int32, docs.shape, 1)
    return jnp.sum(jnp.where(lane == me, docs, 0.0), axis=1, keepdims=True)


def key_doc(docs_ref, block, me):
    row = docs_ref[pl.ds(jnp.maximum(block, 0), 1), :]
    return jnp.where((block >= 0) & (block <= me), row, -1.0)


def stack(q_ref, h, group):
    return jnp.concatenate(
        [q_ref[:, pl.ds((h * group + g) * HD, HD)] for g in range(group)], axis=0
    )


def scores_of(queries, keys):
    return lax.dot_general(
        queries, keys, (((1,), (1,)), ((), ())), preferred_element_type=jnp.float32
    )


def early_kernel(kv_local, group, count, step, *refs):
    q_ref, docs_ref, docs_t_ref = refs[:3]
    blocks = refs[3 : 3 + count]
    acc_ref, top_ref, sum_ref = refs[3 + count : 6 + count]
    bias_ref, s_ref, p_ref = refs[6 + count :]
    tokens = q_ref.shape[0]
    stacked = group * tokens
    me = lax.axis_index("seq")
    row, col = me // 2, me % 2
    docs = []
    for i in range(count):
        block = me - i if i % 2 == 0 else (row - i // 2) * 2 + 1 - col
        docs.append(key_doc(docs_ref, block, me))
    allowed = query_doc(docs_t_ref, me) == jnp.concatenate(docs, axis=1)
    key_at = lax.broadcasted_iota(jnp.int32, (tokens, count * tokens), 1)
    query_at = lax.broadcasted_iota(jnp.int32, (tokens, count * tokens), 0)
    allowed = allowed & ((key_at <= query_at) | (key_at >= tokens))
    bias_ref[...] = jnp.where(allowed, 0.0, -jnp.inf)
    for h in range(kv_local):
        keys = jnp.concatenate([b[:, pl.ds(h * HD, HD)] for b in blocks], axis=0)
        s_ref[...] = scores_of(stack(q_ref, h, group), keys)
        for r in range(0, stacked, step):
            at = pl.ds(r, step)
            into = pl.ds(h * stacked + r, step)
            scores = s_ref[at, :] * SCALE + bias_ref[pl.ds(r % tokens, step), :]
            top = jnp.max(scores, axis=-1, keepdims=True)
            weight = jnp.exp2(scores - top)
            total = jnp.sum(weight, axis=-1, keepdims=True)
            p_ref[at, :] = weight.astype(jnp.bfloat16)
            top_ref[into, :] = jnp.broadcast_to(top, (step, HD))
            sum_ref[into, :] = jnp.broadcast_to(total, (step, HD))
        cols = pl.ds((kv_local + h) * HD, HD)
        values = jnp.concatenate([b[:, cols] for b in blocks], axis=0)
        acc_ref[pl.ds(h * stacked, stacked), :] = jnp.dot(
            p_ref[...], values, preferred_element_type=jnp.float32
        )


def project(context_ref, w_ref, start, width, send_ref, keep_ref, part):
    step = 256
    for c in range(0, width, step):
        at = pl.ds(c, step)
        rows = jnp.dot(
            context_ref[...],
            w_ref[:, pl.ds(start + c, step)],
            preferred_element_type=jnp.float32,
        ).astype(jnp.bfloat16)
        for i in range(rows.shape[0] // (2 * part)):
            into = pl.ds(i * part, part)
            keep_ref[into, at] = rows[2 * i * part : (2 * i + 1) * part]
            send_ref[into, at] = rows[(2 * i + 1) * part : (2 * i + 2) * part]


def late_kernel(kv_local, group, part, depth, *refs):
    q_ref, docs_ref, docs_t_ref, block, acc_ref, top_ref, sum_ref, w_ref = refs[:8]
    out_ref, send_ref, keep_ref, context_ref = refs[8:]
    tokens = q_ref.shape[0]
    stacked = group * tokens
    me, rank = lax.axis_index("seq"), lax.axis_index("tp")
    chips = lax.axis_size("tp") // 2
    far = (me // 2 - depth) * 2 + 1 - me % 2
    bias = jnp.where(
        query_doc(docs_t_ref, me) == key_doc(docs_ref, far, me), 0.0, -jnp.inf
    )
    for h in range(kv_local):
        keys = block[:, pl.ds(h * HD, HD)]
        values = block[:, pl.ds((kv_local + h) * HD, HD)]
        scores = scores_of(stack(q_ref, h, group), keys)
        scores = scores * SCALE + jnp.concatenate([bias] * group, axis=0)
        at = pl.ds(h * stacked, stacked)
        old = top_ref[at, :]
        new = jnp.maximum(old[:, :1], jnp.max(scores, axis=-1, keepdims=True))
        weight = jnp.exp2(scores - new)
        rescale = jnp.exp2(old - new)
        total = sum_ref[at, :] * rescale + jnp.sum(weight, axis=-1, keepdims=True)
        added = jnp.dot(
            weight.astype(jnp.bfloat16), values, preferred_element_type=jnp.float32
        )
        context = (acc_ref[at, :] * rescale + added) / total
        context = context.astype(jnp.bfloat16)
        for g in range(group):
            cols = pl.ds((h * group + g) * HD, HD)
            context_ref[:, cols] = context[g * tokens : (g + 1) * tokens]
    at = 0
    for distance in range(1, chips + 1):
        base = lax.rem(rank // 2 + distance, chips) * 2
        for core in (rank % 2, 1 - rank % 2):
            first = pl.multiple_of((base + core) * part, 8)
            out_ref[pl.ds(at, part), :] = context_ref[pl.ds(first, part), :]
            at += part
    project(out_ref, w_ref, 0, send_ref.shape[1], send_ref, keep_ref, part)


def project_kernel(part, start, context_ref, w_ref, send_ref, keep_ref):
    width = send_ref.shape[1]
    project(context_ref, w_ref, start, width, send_ref, keep_ref, part)


def project_call(context, weight, start, width, part):
    tokens, depth = context.shape
    out = jax.ShapeDtypeStruct((tokens // 2, width), jnp.bfloat16)
    return pl.pallas_call(
        functools.partial(project_kernel, part, start),
        out_shape=(out, out),
        in_specs=[VMEM, VMEM],
        out_specs=(VMEM, VMEM),
        cost_estimate=pl.CostEstimate(
            flops=2 * tokens * depth * width,
            transcendentals=0,
            bytes_accessed=2 * depth * width,
        ),
        compiler_params=pltpu.CompilerParams(vmem_limit_bytes=8 * MIB),
        name="project_rest",
    )(context, weight)


def layer(query_rows, key_rows, value_rows, document_ids, output_weight):
    tokens = query_rows.shape[0]
    kv_local = key_rows.shape[1] // HD
    group = HEADS // KV
    width = query_rows.shape[1]
    model = output_weight.shape[1]
    seq, tp = lax.axis_size("seq"), lax.axis_size("tp")
    part = tokens // tp
    chips = tp // 2
    reach = min(12, seq // 2)
    depth = (reach + 1) // 2
    route = routes(seq, tp, depth)
    odd_row = (lax.axis_index("seq") // 2) % 2 == 1

    def send(x, name, step):
        return lax.ppermute(x, AXES, route[name, step])

    own = pl.pallas_call(
        join_kernel,
        out_shape=pltpu.VMEM((tokens, 2 * kv_local * HD), jnp.bfloat16),
        in_specs=[ANY, ANY],
        out_specs=VMEM,
        scratch_shapes=[pltpu.SemaphoreType.DMA((2,))],
        compiler_params=pltpu.CompilerParams(vmem_limit_bytes=2 * MIB),
        name="join",
    )(in_hbm(key_rows), in_hbm(value_rows))
    docs = document_ids.astype(jnp.float32).reshape(seq, tokens)
    docs_t = docs.T
    cuts = [model * 7 // 32, model * 17 // 32, model]
    weight = in_hbm(output_weight)
    near_weight = load_call(weight, 0, cuts[1])
    far_weight = load_call(weight, cuts[1], model)
    even, odd = send(own, "even", 1), send(own, "odd", 1)
    blocks = [own, send(own, "col", 0)]
    even, odd, docs, docs_t = lax.optimization_barrier((even, odd, docs, docs_t))
    for distance in range(1, depth + 1):
        blocks.append(jnp.where(odd_row, even, odd))
        if distance < depth:
            even, odd = (
                send(odd, "even", distance + 1),
                send(even, "odd", distance + 1),
            )
        blocks.append(send(blocks[-1], "col", distance))
    last_block = blocks.pop()
    count = len(blocks)

    stacked = group * tokens
    state = jax.ShapeDtypeStruct((kv_local * stacked, HD), jnp.float32)
    acc, top, total = pl.pallas_call(
        functools.partial(early_kernel, kv_local, group, count, 32),
        out_shape=(state, state, state),
        in_specs=[VMEM] * (3 + count),
        out_specs=(VMEM,) * 3,
        scratch_shapes=[
            pltpu.VMEM((tokens, count * tokens), jnp.float32),
            pltpu.VMEM((stacked, count * tokens), jnp.float32),
            pltpu.VMEM((stacked, count * tokens), jnp.bfloat16),
        ],
        cost_estimate=pl.CostEstimate(
            flops=4 * tokens * tokens * count * width,
            transcendentals=tokens * tokens * count * width // HD,
            bytes_accessed=4 * tokens * width,
        ),
        compiler_params=pltpu.CompilerParams(vmem_limit_bytes=24 * MIB),
        name="attend_early",
    )(query_rows, docs, docs_t, *blocks)

    out = jax.ShapeDtypeStruct((tokens // 2, cuts[0]), jnp.bfloat16)
    context, sent, kept = pl.pallas_call(
        functools.partial(late_kernel, kv_local, group, part, depth),
        out_shape=(jax.ShapeDtypeStruct((tokens, width), jnp.bfloat16), out, out),
        in_specs=[VMEM] * 8,
        out_specs=(VMEM, VMEM, VMEM),
        scratch_shapes=[pltpu.VMEM((tokens, width), jnp.bfloat16)],
        cost_estimate=pl.CostEstimate(
            flops=4 * tokens * tokens * width + 2 * tokens * width * cuts[0],
            transcendentals=tokens * tokens * width // HD,
            bytes_accessed=4 * tokens * width + 2 * width * cuts[0],
        ),
        compiler_params=pltpu.CompilerParams(vmem_limit_bytes=16 * MIB),
        name="attend_late",
    )(query_rows, docs, docs_t, last_block, acc, top, total, near_weight)

    pieces = []
    remote = (chips - 1) * part
    for i, stop in enumerate(cuts):
        if i:
            from_weight = near_weight if i == 1 else far_weight
            start = cuts[0] if i == 1 else 0
            sent, kept = project_call(
                context, from_weight, start, stop - cuts[i - 1], part
            )
        received = send(sent, "core", i)
        moved = (
            kept[:remote].astype(jnp.float32) + received[:remote].astype(jnp.float32)
        ).astype(jnp.bfloat16)
        piece = kept[remote:].astype(jnp.float32) + received[remote:].astype(
            jnp.float32
        )
        for distance in range(1, chips):
            at = (distance - 1) * part
            arrived = lax.ppermute(
                moved[at : at + part], AXES, y_route(seq, tp, distance)
            )
            piece = piece + arrived.astype(jnp.float32)
        pieces.append(piece.astype(jnp.bfloat16))
    return jnp.concatenate(pieces, axis=1)


def solution(mesh):
    in_specs = (P("seq", "tp"), P("seq", "tp"), P("seq", "tp"), P(), P("tp", None))
    out_specs = P(("seq", "tp"), None)
    return jax.shard_map(
        layer, mesh=mesh, in_specs=in_specs, out_specs=out_specs, check_vma=False
    )
```

```python
import functools

import jax
import jax.numpy as jnp
from jax import lax
from jax.experimental import pallas as pl
from jax.experimental.pallas import tpu as pltpu
from jax.sharding import PartitionSpec as P


HEADS = 32
KV = 8
HD = 128
AXES = ("seq", "tp")
LOG2E = 1.4426950408889634
SCALE = LOG2E / HD**0.5
VMEM = pl.BlockSpec(memory_space=pltpu.VMEM)
ANY = pl.BlockSpec(memory_space=pl.ANY)
MIB = 1 << 20
CUTS = (7, 17, 32)
NEAR = 12
EARLY, LATE, PROJ = 24, 16, 8


def routes(seq, tp, depth):
    rows = seq // 2

    def flat(rule):
        pairs = []
        for s in range(seq):
            for t in range(tp):
                s2, t2 = rule(s, t)
                pairs.append((s * tp + t, s2 * tp + t2))
        return pairs

    def by_row(parity, step):
        def rule(s, t):
            row, col = divmod(s, 2)
            other = row + 1 if row % 2 == parity else row - 1
            if step - 1 <= min(row, other) and max(row, other) < rows:
                return other * 2 + col, t
            return s, t ^ 1

        return flat(rule)

    def by_col(step):
        return flat(lambda s, t: (s ^ 1, t) if s // 2 >= step else (s, t ^ 1))

    table = {("core", i): flat(lambda s, t: (s, t ^ 1)) for i in range(len(CUTS))}
    for step in range(depth + 1):
        table["col", step] = by_col(step)
        table["even", step] = by_row(0, step)
        table["odd", step] = by_row(1, step)
    return table


def y_route(seq, tp, distance):
    pairs = []
    for s in range(seq):
        for t in range(tp):
            pairs.append((s * tp + t, s * tp + (t + 2 * distance) % tp))
    return pairs


def join_kernel(k_ref, v_ref, out_ref, sems):
    width = k_ref.shape[1]
    copies = [
        pltpu.make_async_copy(k_ref, out_ref.at[:, pl.ds(0, width)], sems.at[0]),
        pltpu.make_async_copy(v_ref, out_ref.at[:, pl.ds(width, width)], sems.at[1]),
    ]
    for copy in copies:
        copy.start()
    for copy in copies:
        copy.wait()


def load_kernel(start, w_hbm, *refs):
    *outs, sems = refs
    copies = []
    for i, out in enumerate(outs):
        width = out.shape[1]
        source = w_hbm.at[:, pl.ds(start, width)]
        copies.append(pltpu.make_async_copy(source, out, sems.at[i]))
        start += width
    for copy in copies:
        copy.start()
    for copy in copies:
        copy.wait()


def load_call(weight, cuts):
    depth = weight.shape[0]
    widths = [stop - start for start, stop in zip(cuts, cuts[1:])]
    return pl.pallas_call(
        functools.partial(load_kernel, cuts[0]),
        out_shape=[pltpu.VMEM((depth, width), weight.dtype) for width in widths],
        in_specs=[ANY],
        out_specs=[VMEM] * len(widths),
        scratch_shapes=[pltpu.SemaphoreType.DMA((len(widths),))],
        cost_estimate=pl.CostEstimate(
            flops=0,
            transcendentals=0,
            bytes_accessed=2 * depth * (cuts[-1] - cuts[0]),
        ),
        compiler_params=pltpu.CompilerParams(vmem_limit_bytes=MIB),
        name="load",
    )(weight)


def in_hbm(x):
    return pltpu.with_memory_space_constraint(x, pltpu.HBM)


def query_doc(docs_ref, me):
    docs = docs_ref[...]
    own = lax.broadcasted_iota(jnp.int32, (docs.shape[0], HD), 0) == me
    column = lax.dot_general(
        docs,
        own.astype(jnp.float32),
        (((0,), (0,)), ((), ())),
        precision=lax.Precision.HIGHEST,
        preferred_element_type=jnp.float32,
    )
    return column[:, :1]


def key_doc(docs_ref, block, me):
    row = docs_ref[pl.ds(jnp.maximum(block, 0), 1), :]
    return jnp.where((block >= 0) & (block <= me), row, -1.0)


def stack(q_ref, h, group):
    return jnp.concatenate(
        [q_ref[:, pl.ds((h * group + g) * HD, HD)] for g in range(group)], axis=0
    )


def scores_of(queries, keys):
    return lax.dot_general(
        queries, keys, (((1,), (1,)), ((), ())), preferred_element_type=jnp.float32
    )


def early_kernel(kv_local, group, count, step, *refs):
    q_ref, docs_ref = refs[:2]
    blocks = refs[2 : 2 + count]
    acc_ref, top_ref, sum_ref = refs[2 + count : 5 + count]
    bias_ref, s_ref, p_ref = refs[5 + count :]
    tokens = q_ref.shape[0]
    stacked = group * tokens
    me = lax.axis_index("seq")
    row, col = me // 2, me % 2
    docs = []
    for i in range(count):
        block = me - i if i % 2 == 0 else (row - i // 2) * 2 + 1 - col
        docs.append(key_doc(docs_ref, block, me))
    allowed = query_doc(docs_ref, me) == jnp.concatenate(docs, axis=1)
    key_at = lax.broadcasted_iota(jnp.int32, (tokens, count * tokens), 1)
    query_at = lax.broadcasted_iota(jnp.int32, (tokens, count * tokens), 0)
    allowed = allowed & ((key_at <= query_at) | (key_at >= tokens))
    bias_ref[...] = jnp.where(allowed, 0.0, -jnp.inf)
    for h in range(kv_local):
        keys = jnp.concatenate([b[:, pl.ds(h * HD, HD)] for b in blocks], axis=0)
        s_ref[...] = scores_of(stack(q_ref, h, group), keys)
        for r in range(0, stacked, step):
            at = pl.ds(r, step)
            into = pl.ds(h * stacked + r, step)
            scores = s_ref[at, :] * SCALE + bias_ref[pl.ds(r % tokens, step), :]
            top = jnp.max(scores, axis=-1, keepdims=True)
            weight = jnp.exp2(scores - top)
            total = jnp.sum(weight, axis=-1, keepdims=True)
            p_ref[at, :] = weight.astype(jnp.bfloat16)
            top_ref[into, :] = jnp.broadcast_to(top, (step, HD))
            sum_ref[into, :] = jnp.broadcast_to(total, (step, HD))
        cols = pl.ds((kv_local + h) * HD, HD)
        values = jnp.concatenate([b[:, cols] for b in blocks], axis=0)
        acc_ref[pl.ds(h * stacked, stacked), :] = jnp.dot(
            p_ref[...], values, preferred_element_type=jnp.float32
        )


def project(context_ref, w_ref, send_ref, keep_ref, part):
    step = 256
    for c in range(0, w_ref.shape[1], step):
        at = pl.ds(c, step)
        rows = jnp.dot(
            context_ref[...],
            w_ref[:, at],
            preferred_element_type=jnp.float32,
        ).astype(jnp.bfloat16)
        for i in range(rows.shape[0] // (2 * part)):
            into = pl.ds(i * part, part)
            keep_ref[into, at] = rows[2 * i * part : (2 * i + 1) * part]
            send_ref[into, at] = rows[(2 * i + 1) * part : (2 * i + 2) * part]


def late_kernel(kv_local, group, part, depth, *refs):
    q_ref, docs_ref, block, acc_ref, top_ref, sum_ref, w_ref = refs[:7]
    out_ref, send_ref, keep_ref, context_ref = refs[7:]
    tokens = q_ref.shape[0]
    stacked = group * tokens
    me, rank = lax.axis_index("seq"), lax.axis_index("tp")
    chips = lax.axis_size("tp") // 2
    far = (me // 2 - depth) * 2 + 1 - me % 2
    bias = jnp.where(
        query_doc(docs_ref, me) == key_doc(docs_ref, far, me), 0.0, -jnp.inf
    )
    for h in range(kv_local):
        keys = block[:, pl.ds(h * HD, HD)]
        values = block[:, pl.ds((kv_local + h) * HD, HD)]
        scores = scores_of(stack(q_ref, h, group), keys)
        scores = scores * SCALE + jnp.concatenate([bias] * group, axis=0)
        at = pl.ds(h * stacked, stacked)
        old = top_ref[at, :]
        new = jnp.maximum(old[:, :1], jnp.max(scores, axis=-1, keepdims=True))
        weight = jnp.exp2(scores - new)
        rescale = jnp.exp2(old - new)
        total = sum_ref[at, :] * rescale + jnp.sum(weight, axis=-1, keepdims=True)
        added = jnp.dot(
            weight.astype(jnp.bfloat16), values, preferred_element_type=jnp.float32
        )
        context = (acc_ref[at, :] * rescale + added) / total
        context = context.astype(jnp.bfloat16)
        for g in range(group):
            cols = pl.ds((h * group + g) * HD, HD)
            context_ref[:, cols] = context[g * tokens : (g + 1) * tokens]
    at = 0
    for distance in range(1, chips + 1):
        base = lax.rem(rank // 2 + distance, chips) * 2
        for core in (rank % 2, 1 - rank % 2):
            first = pl.multiple_of((base + core) * part, 8)
            out_ref[pl.ds(at, part), :] = context_ref[pl.ds(first, part), :]
            at += part
    project(out_ref, w_ref, send_ref, keep_ref, part)


def project_kernel(part, context_ref, *refs):
    *weights, send_ref, keep_ref = refs
    start = 0
    for w_ref in weights:
        cols = pl.ds(start, w_ref.shape[1])
        project(context_ref, w_ref, send_ref.at[:, cols], keep_ref.at[:, cols], part)
        start += w_ref.shape[1]


def project_call(context, weights, part):
    tokens, depth = context.shape
    width = sum(weight.shape[1] for weight in weights)
    out = jax.ShapeDtypeStruct((tokens // 2, width), jnp.bfloat16)
    return pl.pallas_call(
        functools.partial(project_kernel, part),
        out_shape=(out, out),
        in_specs=[VMEM] * (1 + len(weights)),
        out_specs=(VMEM, VMEM),
        cost_estimate=pl.CostEstimate(
            flops=2 * tokens * depth * width,
            transcendentals=0,
            bytes_accessed=2 * depth * width,
        ),
        compiler_params=pltpu.CompilerParams(vmem_limit_bytes=PROJ * MIB),
        name="project_rest",
    )(context, *weights)


def layer(query_rows, key_rows, value_rows, document_ids, output_weight):
    tokens = query_rows.shape[0]
    kv_local = key_rows.shape[1] // HD
    group = HEADS // KV
    width = query_rows.shape[1]
    model = output_weight.shape[1]
    seq, tp = lax.axis_size("seq"), lax.axis_size("tp")
    part = tokens // tp
    chips = tp // 2
    reach = min(12, seq // 2)
    depth = (reach + 1) // 2
    route = routes(seq, tp, depth)
    odd_row = (lax.axis_index("seq") // 2) % 2 == 1

    def send(x, name, step):
        return lax.ppermute(x, AXES, route[name, step])

    own = pl.pallas_call(
        join_kernel,
        out_shape=pltpu.VMEM((tokens, 2 * kv_local * HD), jnp.bfloat16),
        in_specs=[ANY, ANY],
        out_specs=VMEM,
        scratch_shapes=[pltpu.SemaphoreType.DMA((2,))],
        compiler_params=pltpu.CompilerParams(vmem_limit_bytes=2 * MIB),
        name="join",
    )(in_hbm(key_rows), in_hbm(value_rows))
    docs = document_ids.astype(jnp.float32).reshape(seq, tokens)
    cuts = [model * n // 32 for n in (0, *CUTS)]
    near = model * NEAR // 32
    weight = in_hbm(output_weight)
    first, *middle = load_call(weight, (0, cuts[1], near))
    *rest, last = load_call(weight, (near, *cuts[2:]))
    weights = [[first], middle + rest, [last]]
    even, odd = send(own, "even", 1), send(own, "odd", 1)
    blocks = [own, send(own, "col", 0)]
    even, odd, docs = lax.optimization_barrier((even, odd, docs))
    for distance in range(1, depth + 1):
        blocks.append(jnp.where(odd_row, even, odd))
        if distance < depth:
            even, odd = (
                send(odd, "even", distance + 1),
                send(even, "odd", distance + 1),
            )
        blocks.append(send(blocks[-1], "col", distance))
    last_block = blocks.pop()
    count = len(blocks)

    stacked = group * tokens
    state = jax.ShapeDtypeStruct((kv_local * stacked, HD), jnp.float32)
    acc, top, total = pl.pallas_call(
        functools.partial(early_kernel, kv_local, group, count, 32),
        out_shape=(state, state, state),
        in_specs=[VMEM] * (2 + count),
        out_specs=(VMEM,) * 3,
        scratch_shapes=[
            pltpu.VMEM((tokens, count * tokens), jnp.float32),
            pltpu.VMEM((stacked, count * tokens), jnp.float32),
            pltpu.VMEM((stacked, count * tokens), jnp.bfloat16),
        ],
        cost_estimate=pl.CostEstimate(
            flops=4 * tokens * tokens * count * width,
            transcendentals=tokens * tokens * count * width // HD,
            bytes_accessed=4 * tokens * width,
        ),
        compiler_params=pltpu.CompilerParams(vmem_limit_bytes=EARLY * MIB),
        name="attend_early",
    )(query_rows, docs, *blocks)

    out = jax.ShapeDtypeStruct((tokens // 2, cuts[1]), jnp.bfloat16)
    context, sent, kept = pl.pallas_call(
        functools.partial(late_kernel, kv_local, group, part, depth),
        out_shape=(jax.ShapeDtypeStruct((tokens, width), jnp.bfloat16), out, out),
        in_specs=[VMEM] * 7,
        out_specs=(VMEM, VMEM, VMEM),
        scratch_shapes=[pltpu.VMEM((tokens, width), jnp.bfloat16)],
        cost_estimate=pl.CostEstimate(
            flops=4 * tokens * tokens * width + 2 * tokens * width * cuts[1],
            transcendentals=tokens * tokens * width // HD,
            bytes_accessed=4 * tokens * width + 2 * width * cuts[1],
        ),
        compiler_params=pltpu.CompilerParams(vmem_limit_bytes=LATE * MIB),
        name="attend_late",
    )(query_rows, docs, last_block, acc, top, total, first)

    pieces = []
    remote = (chips - 1) * part
    for i, weight in enumerate(weights):
        if i:
            sent, kept = project_call(context, weight, part)
        received = send(sent, "core", i)
        moved = (
            kept[:remote].astype(jnp.float32) + received[:remote].astype(jnp.float32)
        ).astype(jnp.bfloat16)
        piece = kept[remote:].astype(jnp.float32) + received[remote:].astype(
            jnp.float32
        )
        for distance in range(1, chips):
            at = (distance - 1) * part
            arrived = lax.ppermute(
                moved[at : at + part], AXES, y_route(seq, tp, distance)
            )
            piece = piece + arrived.astype(jnp.float32)
        pieces.append(piece.astype(jnp.bfloat16))
    return jnp.concatenate(pieces, axis=1)


def solution(mesh):
    in_specs = (P("seq", "tp"), P("seq", "tp"), P("seq", "tp"), P(), P("tp", None))
    out_specs = P(("seq", "tp"), None)
    return jax.shard_map(
        layer, mesh=mesh, in_specs=in_specs, out_specs=out_specs, check_vma=False
    )
```

```python
import functools

import jax
import jax.numpy as jnp
from jax import lax
from jax.experimental import pallas as pl
from jax.experimental.pallas import tpu as pltpu
from jax.sharding import PartitionSpec as P


HEADS = 32
KV = 8
HD = 128
AXES = ("seq", "tp")
LOG2E = 1.4426950408889634
SCALE = LOG2E / HD**0.5
VMEM = pl.BlockSpec(memory_space=pltpu.VMEM)
ANY = pl.BlockSpec(memory_space=pl.ANY)
MIB = 1 << 20
CUTS = (7, 17, 24, 32)
NEAR = 12
EARLY, LATE, PROJ = 24, 16, 8


def routes(seq, tp, depth):
    rows = seq // 2

    def flat(rule):
        pairs = []
        for s in range(seq):
            for t in range(tp):
                s2, t2 = rule(s, t)
                pairs.append((s * tp + t, s2 * tp + t2))
        return pairs

    def by_row(parity, step):
        def rule(s, t):
            row, col = divmod(s, 2)
            other = row + 1 if row % 2 == parity else row - 1
            if step - 1 <= min(row, other) and max(row, other) < rows:
                return other * 2 + col, t
            return s, t ^ 1

        return flat(rule)

    def by_col(step):
        return flat(lambda s, t: (s ^ 1, t) if s // 2 >= step else (s, t ^ 1))

    table = {("core", i): flat(lambda s, t: (s, t ^ 1)) for i in range(len(CUTS))}
    for step in range(depth + 1):
        table["col", step] = by_col(step)
        table["even", step] = by_row(0, step)
        table["odd", step] = by_row(1, step)
    return table


def y_route(seq, tp, distance):
    pairs = []
    for s in range(seq):
        for t in range(tp):
            pairs.append((s * tp + t, s * tp + (t + 2 * distance) % tp))
    return pairs


def join_kernel(k_ref, v_ref, out_ref, sems):
    width = k_ref.shape[1]
    copies = [
        pltpu.make_async_copy(k_ref, out_ref.at[:, pl.ds(0, width)], sems.at[0]),
        pltpu.make_async_copy(v_ref, out_ref.at[:, pl.ds(width, width)], sems.at[1]),
    ]
    for copy in copies:
        copy.start()
    for copy in copies:
        copy.wait()


def load_kernel(start, w_hbm, *refs):
    *outs, sems = refs
    copies = []
    for i, out in enumerate(outs):
        width = out.shape[1]
        source = w_hbm.at[:, pl.ds(start, width)]
        copies.append(pltpu.make_async_copy(source, out, sems.at[i]))
        start += width
    for copy in copies:
        copy.start()
    for copy in copies:
        copy.wait()


def load_call(weight, cuts):
    depth = weight.shape[0]
    widths = [stop - start for start, stop in zip(cuts, cuts[1:])]
    return pl.pallas_call(
        functools.partial(load_kernel, cuts[0]),
        out_shape=[pltpu.VMEM((depth, width), weight.dtype) for width in widths],
        in_specs=[ANY],
        out_specs=[VMEM] * len(widths),
        scratch_shapes=[pltpu.SemaphoreType.DMA((len(widths),))],
        cost_estimate=pl.CostEstimate(
            flops=0,
            transcendentals=0,
            bytes_accessed=2 * depth * (cuts[-1] - cuts[0]),
        ),
        compiler_params=pltpu.CompilerParams(vmem_limit_bytes=MIB),
        name="load",
    )(weight)


def in_hbm(x):
    return pltpu.with_memory_space_constraint(x, pltpu.HBM)


def query_doc(docs_ref, me):
    docs = docs_ref[...]
    own = lax.broadcasted_iota(jnp.int32, (docs.shape[0], HD), 0) == me
    column = lax.dot_general(
        docs,
        own.astype(jnp.float32),
        (((0,), (0,)), ((), ())),
        precision=lax.Precision.HIGHEST,
        preferred_element_type=jnp.float32,
    )
    return column[:, :1]


def key_doc(docs_ref, block, me):
    row = docs_ref[pl.ds(jnp.maximum(block, 0), 1), :]
    return jnp.where((block >= 0) & (block <= me), row, -1.0)


def stack(q_ref, h, group):
    return jnp.concatenate(
        [q_ref[:, pl.ds((h * group + g) * HD, HD)] for g in range(group)], axis=0
    )


def scores_of(queries, keys):
    return lax.dot_general(
        queries, keys, (((1,), (1,)), ((), ())), preferred_element_type=jnp.float32
    )


def early_kernel(kv_local, group, count, step, *refs):
    q_ref, docs_ref = refs[:2]
    blocks = refs[2 : 2 + count]
    acc_ref, top_ref, sum_ref = refs[2 + count : 5 + count]
    bias_ref, s_ref, p_ref = refs[5 + count :]
    tokens = q_ref.shape[0]
    stacked = group * tokens
    me = lax.axis_index("seq")
    row, col = me // 2, me % 2
    docs = []
    for i in range(count):
        block = me - i if i % 2 == 0 else (row - i // 2) * 2 + 1 - col
        docs.append(key_doc(docs_ref, block, me))
    allowed = query_doc(docs_ref, me) == jnp.concatenate(docs, axis=1)
    key_at = lax.broadcasted_iota(jnp.int32, (tokens, count * tokens), 1)
    query_at = lax.broadcasted_iota(jnp.int32, (tokens, count * tokens), 0)
    allowed = allowed & ((key_at <= query_at) | (key_at >= tokens))
    bias_ref[...] = jnp.where(allowed, 0.0, -jnp.inf)
    for h in range(kv_local):
        keys = jnp.concatenate([b[:, pl.ds(h * HD, HD)] for b in blocks], axis=0)
        s_ref[...] = scores_of(stack(q_ref, h, group), keys)
        for r in range(0, stacked, step):
            at = pl.ds(r, step)
            into = pl.ds(h * stacked + r, step)
            scores = s_ref[at, :] * SCALE + bias_ref[pl.ds(r % tokens, step), :]
            top = jnp.max(scores, axis=-1, keepdims=True)
            weight = jnp.exp2(scores - top)
            total = jnp.sum(weight, axis=-1, keepdims=True)
            p_ref[at, :] = weight.astype(jnp.bfloat16)
            top_ref[into, :] = jnp.broadcast_to(top, (step, HD))
            sum_ref[into, :] = jnp.broadcast_to(total, (step, HD))
        cols = pl.ds((kv_local + h) * HD, HD)
        values = jnp.concatenate([b[:, cols] for b in blocks], axis=0)
        acc_ref[pl.ds(h * stacked, stacked), :] = jnp.dot(
            p_ref[...], values, preferred_element_type=jnp.float32
        )


def project(context_ref, w_ref, send_ref, keep_ref, part):
    step = 256
    for c in range(0, w_ref.shape[1], step):
        at = pl.ds(c, step)
        rows = jnp.dot(
            context_ref[...],
            w_ref[:, at],
            preferred_element_type=jnp.float32,
        ).astype(jnp.bfloat16)
        for i in range(rows.shape[0] // (2 * part)):
            into = pl.ds(i * part, part)
            keep_ref[into, at] = rows[2 * i * part : (2 * i + 1) * part]
            send_ref[into, at] = rows[(2 * i + 1) * part : (2 * i + 2) * part]


def late_kernel(kv_local, group, part, depth, *refs):
    q_ref, docs_ref, block, acc_ref, top_ref, sum_ref, w_ref = refs[:7]
    out_ref, send_ref, keep_ref, context_ref = refs[7:]
    tokens = q_ref.shape[0]
    stacked = group * tokens
    me, rank = lax.axis_index("seq"), lax.axis_index("tp")
    chips = lax.axis_size("tp") // 2
    far = (me // 2 - depth) * 2 + 1 - me % 2
    bias = jnp.where(
        query_doc(docs_ref, me) == key_doc(docs_ref, far, me), 0.0, -jnp.inf
    )
    for h in range(kv_local):
        keys = block[:, pl.ds(h * HD, HD)]
        values = block[:, pl.ds((kv_local + h) * HD, HD)]
        scores = scores_of(stack(q_ref, h, group), keys)
        scores = scores * SCALE + jnp.concatenate([bias] * group, axis=0)
        at = pl.ds(h * stacked, stacked)
        old = top_ref[at, :]
        new = jnp.maximum(old[:, :1], jnp.max(scores, axis=-1, keepdims=True))
        weight = jnp.exp2(scores - new)
        rescale = jnp.exp2(old - new)
        total = sum_ref[at, :] * rescale + jnp.sum(weight, axis=-1, keepdims=True)
        added = jnp.dot(
            weight.astype(jnp.bfloat16), values, preferred_element_type=jnp.float32
        )
        context = (acc_ref[at, :] * rescale + added) / total
        context = context.astype(jnp.bfloat16)
        for g in range(group):
            cols = pl.ds((h * group + g) * HD, HD)
            context_ref[:, cols] = context[g * tokens : (g + 1) * tokens]
    at = 0
    for distance in range(1, chips + 1):
        base = lax.rem(rank // 2 + distance, chips) * 2
        for core in (rank % 2, 1 - rank % 2):
            first = pl.multiple_of((base + core) * part, 8)
            out_ref[pl.ds(at, part), :] = context_ref[pl.ds(first, part), :]
            at += part
    project(out_ref, w_ref, send_ref, keep_ref, part)


def project_kernel(part, context_ref, *refs):
    *weights, send_ref, keep_ref = refs
    start = 0
    for w_ref in weights:
        cols = pl.ds(start, w_ref.shape[1])
        project(context_ref, w_ref, send_ref.at[:, cols], keep_ref.at[:, cols], part)
        start += w_ref.shape[1]


def project_call(context, weights, part):
    tokens, depth = context.shape
    width = sum(weight.shape[1] for weight in weights)
    out = jax.ShapeDtypeStruct((tokens // 2, width), jnp.bfloat16)
    return pl.pallas_call(
        functools.partial(project_kernel, part),
        out_shape=(out, out),
        in_specs=[VMEM] * (1 + len(weights)),
        out_specs=(VMEM, VMEM),
        cost_estimate=pl.CostEstimate(
            flops=2 * tokens * depth * width,
            transcendentals=0,
            bytes_accessed=2 * depth * width,
        ),
        compiler_params=pltpu.CompilerParams(vmem_limit_bytes=PROJ * MIB),
        name="project_rest",
    )(context, *weights)


def layer(query_rows, key_rows, value_rows, document_ids, output_weight):
    tokens = query_rows.shape[0]
    kv_local = key_rows.shape[1] // HD
    group = HEADS // KV
    width = query_rows.shape[1]
    model = output_weight.shape[1]
    seq, tp = lax.axis_size("seq"), lax.axis_size("tp")
    part = tokens // tp
    chips = tp // 2
    reach = min(12, seq // 2)
    depth = (reach + 1) // 2
    route = routes(seq, tp, depth)
    odd_row = (lax.axis_index("seq") // 2) % 2 == 1

    def send(x, name, step):
        return lax.ppermute(x, AXES, route[name, step])

    own = pl.pallas_call(
        join_kernel,
        out_shape=pltpu.VMEM((tokens, 2 * kv_local * HD), jnp.bfloat16),
        in_specs=[ANY, ANY],
        out_specs=VMEM,
        scratch_shapes=[pltpu.SemaphoreType.DMA((2,))],
        compiler_params=pltpu.CompilerParams(vmem_limit_bytes=2 * MIB),
        name="join",
    )(in_hbm(key_rows), in_hbm(value_rows))
    docs = document_ids.astype(jnp.float32).reshape(seq, tokens)
    cuts = [model * n // 32 for n in (0, *CUTS)]
    near = model * NEAR // 32
    weight = in_hbm(output_weight)
    first, *middle = load_call(weight, (0, cuts[1], near))
    *rest, third = load_call(weight, (near, *cuts[2:4]))
    weights = [[first], middle + rest, [third]]
    weights.append(load_call(weight, cuts[3:]))
    even, odd = send(own, "even", 1), send(own, "odd", 1)
    blocks = [own, send(own, "col", 0)]
    even, odd, docs = lax.optimization_barrier((even, odd, docs))
    for distance in range(1, depth + 1):
        blocks.append(jnp.where(odd_row, even, odd))
        if distance < depth:
            even, odd = (
                send(odd, "even", distance + 1),
                send(even, "odd", distance + 1),
            )
        blocks.append(send(blocks[-1], "col", distance))
    last_block = blocks.pop()
    count = len(blocks)

    stacked = group * tokens
    state = jax.ShapeDtypeStruct((kv_local * stacked, HD), jnp.float32)
    acc, top, total = pl.pallas_call(
        functools.partial(early_kernel, kv_local, group, count, 32),
        out_shape=(state, state, state),
        in_specs=[VMEM] * (2 + count),
        out_specs=(VMEM,) * 3,
        scratch_shapes=[
            pltpu.VMEM((tokens, count * tokens), jnp.float32),
            pltpu.VMEM((stacked, count * tokens), jnp.float32),
            pltpu.VMEM((stacked, count * tokens), jnp.bfloat16),
        ],
        cost_estimate=pl.CostEstimate(
            flops=4 * tokens * tokens * count * width,
            transcendentals=tokens * tokens * count * width // HD,
            bytes_accessed=4 * tokens * width,
        ),
        compiler_params=pltpu.CompilerParams(vmem_limit_bytes=EARLY * MIB),
        name="attend_early",
    )(query_rows, docs, *blocks)

    out = jax.ShapeDtypeStruct((tokens // 2, cuts[1]), jnp.bfloat16)
    context, sent, kept = pl.pallas_call(
        functools.partial(late_kernel, kv_local, group, part, depth),
        out_shape=(jax.ShapeDtypeStruct((tokens, width), jnp.bfloat16), out, out),
        in_specs=[VMEM] * 7,
        out_specs=(VMEM, VMEM, VMEM),
        scratch_shapes=[pltpu.VMEM((tokens, width), jnp.bfloat16)],
        cost_estimate=pl.CostEstimate(
            flops=4 * tokens * tokens * width + 2 * tokens * width * cuts[1],
            transcendentals=tokens * tokens * width // HD,
            bytes_accessed=4 * tokens * width + 2 * width * cuts[1],
        ),
        compiler_params=pltpu.CompilerParams(vmem_limit_bytes=LATE * MIB),
        name="attend_late",
    )(query_rows, docs, last_block, acc, top, total, first)

    pieces = []
    remote = (chips - 1) * part
    for i, weight in enumerate(weights):
        if i:
            sent, kept = project_call(context, weight, part)
        received = send(sent, "core", i)
        moved = (
            kept[:remote].astype(jnp.float32) + received[:remote].astype(jnp.float32)
        ).astype(jnp.bfloat16)
        piece = kept[remote:].astype(jnp.float32) + received[remote:].astype(
            jnp.float32
        )
        for distance in range(1, chips):
            at = (distance - 1) * part
            arrived = lax.ppermute(
                moved[at : at + part], AXES, y_route(seq, tp, distance)
            )
            piece = piece + arrived.astype(jnp.float32)
        pieces.append(piece.astype(jnp.bfloat16))
    return jnp.concatenate(pieces, axis=1)


def solution(mesh):
    in_specs = (P("seq", "tp"), P("seq", "tp"), P("seq", "tp"), P(), P("tp", None))
    out_specs = P(("seq", "tp"), None)
    return jax.shard_map(
        layer, mesh=mesh, in_specs=in_specs, out_specs=out_specs, check_vma=False
    )
```

```python
import functools

import jax
import jax.numpy as jnp
from jax import lax
from jax.experimental import pallas as pl
from jax.experimental.pallas import tpu as pltpu
from jax.sharding import PartitionSpec as P


HEADS = 32
KV = 8
HD = 128
AXES = ("seq", "tp")
LOG2E = 1.4426950408889634
SCALE = LOG2E / HD**0.5
VMEM = pl.BlockSpec(memory_space=pltpu.VMEM)
ANY = pl.BlockSpec(memory_space=pl.ANY)
MIB = 1 << 20
CUTS = (7, 17, 24, 32)
NEAR = 12
EARLY, LATE, PROJ = 24, 16, 8


def routes(seq, tp, depth):
    rows = seq // 2

    def flat(rule):
        pairs = []
        for s in range(seq):
            for t in range(tp):
                s2, t2 = rule(s, t)
                pairs.append((s * tp + t, s2 * tp + t2))
        return pairs

    def by_row(parity, step):
        def rule(s, t):
            row, col = divmod(s, 2)
            other = row + 1 if row % 2 == parity else row - 1
            if step - 1 <= min(row, other) and max(row, other) < rows:
                return other * 2 + col, t
            return s, t ^ 1

        return flat(rule)

    def by_col(step):
        return flat(lambda s, t: (s ^ 1, t) if s // 2 >= step else (s, t ^ 1))

    table = {("core", i): flat(lambda s, t: (s, t ^ 1)) for i in range(len(CUTS) + 1)}
    for step in range(depth + 1):
        table["col", step] = by_col(step)
        table["even", step] = by_row(0, step)
        table["odd", step] = by_row(1, step)
    return table


def y_route(seq, tp, distance):
    pairs = []
    for s in range(seq):
        for t in range(tp):
            pairs.append((s * tp + t, s * tp + (t + 2 * distance) % tp))
    return pairs


def join_kernel(k_ref, v_ref, out_ref, sems):
    width = k_ref.shape[1]
    copies = [
        pltpu.make_async_copy(k_ref, out_ref.at[:, pl.ds(0, width)], sems.at[0]),
        pltpu.make_async_copy(v_ref, out_ref.at[:, pl.ds(width, width)], sems.at[1]),
    ]
    for copy in copies:
        copy.start()
    for copy in copies:
        copy.wait()


def load_kernel(start, w_hbm, *refs):
    *outs, sems = refs
    copies = []
    for i, out in enumerate(outs):
        width = out.shape[1]
        source = w_hbm.at[:, pl.ds(start, width)]
        copies.append(pltpu.make_async_copy(source, out, sems.at[i]))
        start += width
    for copy in copies:
        copy.start()
    for copy in copies:
        copy.wait()


def load_call(weight, cuts):
    depth = weight.shape[0]
    widths = [stop - start for start, stop in zip(cuts, cuts[1:])]
    return pl.pallas_call(
        functools.partial(load_kernel, cuts[0]),
        out_shape=[pltpu.VMEM((depth, width), weight.dtype) for width in widths],
        in_specs=[ANY],
        out_specs=[VMEM] * len(widths),
        scratch_shapes=[pltpu.SemaphoreType.DMA((len(widths),))],
        cost_estimate=pl.CostEstimate(
            flops=0,
            transcendentals=0,
            bytes_accessed=2 * depth * (cuts[-1] - cuts[0]),
        ),
        compiler_params=pltpu.CompilerParams(vmem_limit_bytes=MIB),
        name="load",
    )(weight)


def in_hbm(x):
    return pltpu.with_memory_space_constraint(x, pltpu.HBM)


def query_doc(docs_ref, me):
    docs = docs_ref[...]
    own = lax.broadcasted_iota(jnp.int32, (docs.shape[0], HD), 0) == me
    column = lax.dot_general(
        docs,
        own.astype(jnp.float32),
        (((0,), (0,)), ((), ())),
        precision=lax.Precision.HIGHEST,
        preferred_element_type=jnp.float32,
    )
    return column[:, :1]


def key_doc(docs_ref, block, me):
    row = docs_ref[pl.ds(jnp.maximum(block, 0), 1), :]
    return jnp.where((block >= 0) & (block <= me), row, -1.0)


def stack(q_ref, h, group):
    return jnp.concatenate(
        [q_ref[:, pl.ds((h * group + g) * HD, HD)] for g in range(group)], axis=0
    )


def scores_of(queries, keys):
    return lax.dot_general(
        queries, keys, (((1,), (1,)), ((), ())), preferred_element_type=jnp.float32
    )


def early_kernel(kv_local, group, count, step, *refs):
    q_ref, docs_ref = refs[:2]
    blocks = refs[2 : 2 + count]
    acc_ref, top_ref, sum_ref = refs[2 + count : 5 + count]
    bias_ref, s_ref, p_ref = refs[5 + count :]
    tokens = q_ref.shape[0]
    stacked = group * tokens
    me = lax.axis_index("seq")
    row, col = me // 2, me % 2
    docs = []
    for i in range(count):
        block = me - i if i % 2 == 0 else (row - i // 2) * 2 + 1 - col
        docs.append(key_doc(docs_ref, block, me))
    allowed = query_doc(docs_ref, me) == jnp.concatenate(docs, axis=1)
    key_at = lax.broadcasted_iota(jnp.int32, (tokens, count * tokens), 1)
    query_at = lax.broadcasted_iota(jnp.int32, (tokens, count * tokens), 0)
    allowed = allowed & ((key_at <= query_at) | (key_at >= tokens))
    bias_ref[...] = jnp.where(allowed, 0.0, -jnp.inf)
    for h in range(kv_local):
        keys = jnp.concatenate([b[:, pl.ds(h * HD, HD)] for b in blocks], axis=0)
        s_ref[...] = scores_of(stack(q_ref, h, group), keys)
        for r in range(0, stacked, step):
            at = pl.ds(r, step)
            into = pl.ds(h * stacked + r, step)
            scores = s_ref[at, :] * SCALE + bias_ref[pl.ds(r % tokens, step), :]
            top = jnp.max(scores, axis=-1, keepdims=True)
            weight = jnp.exp2(scores - top)
            total = jnp.sum(weight, axis=-1, keepdims=True)
            p_ref[at, :] = weight.astype(jnp.bfloat16)
            top_ref[into, :] = jnp.broadcast_to(top, (step, HD))
            sum_ref[into, :] = jnp.broadcast_to(total, (step, HD))
        cols = pl.ds((kv_local + h) * HD, HD)
        values = jnp.concatenate([b[:, cols] for b in blocks], axis=0)
        acc_ref[pl.ds(h * stacked, stacked), :] = jnp.dot(
            p_ref[...], values, preferred_element_type=jnp.float32
        )


def project(context_ref, first, w_ref, send_ref, keep_ref, part):
    step = 256
    count = keep_ref.shape[0] // part
    for c in range(0, w_ref.shape[1], step):
        at = pl.ds(c, step)
        rows = jnp.dot(
            context_ref[pl.ds(first, 2 * count * part), :],
            w_ref[:, at],
            preferred_element_type=jnp.float32,
        ).astype(jnp.bfloat16)
        for i in range(count):
            into = pl.ds(i * part, part)
            keep_ref[into, at] = rows[2 * i * part : (2 * i + 1) * part]
            send_ref[into, at] = rows[(2 * i + 1) * part : (2 * i + 2) * part]


def late_kernel(kv_local, group, part, depth, *refs):
    q_ref, docs_ref, block, acc_ref, top_ref, sum_ref, w_ref = refs[:7]
    out_ref, send_ref, keep_ref, context_ref = refs[7:]
    tokens = q_ref.shape[0]
    stacked = group * tokens
    me, rank = lax.axis_index("seq"), lax.axis_index("tp")
    chips = lax.axis_size("tp") // 2
    far = (me // 2 - depth) * 2 + 1 - me % 2
    bias = jnp.where(
        query_doc(docs_ref, me) == key_doc(docs_ref, far, me), 0.0, -jnp.inf
    )
    for h in range(kv_local):
        keys = block[:, pl.ds(h * HD, HD)]
        values = block[:, pl.ds((kv_local + h) * HD, HD)]
        scores = scores_of(stack(q_ref, h, group), keys)
        scores = scores * SCALE + jnp.concatenate([bias] * group, axis=0)
        at = pl.ds(h * stacked, stacked)
        old = top_ref[at, :]
        new = jnp.maximum(old[:, :1], jnp.max(scores, axis=-1, keepdims=True))
        weight = jnp.exp2(scores - new)
        rescale = jnp.exp2(old - new)
        total = sum_ref[at, :] * rescale + jnp.sum(weight, axis=-1, keepdims=True)
        added = jnp.dot(
            weight.astype(jnp.bfloat16), values, preferred_element_type=jnp.float32
        )
        context = (acc_ref[at, :] * rescale + added) / total
        context = context.astype(jnp.bfloat16)
        for g in range(group):
            cols = pl.ds((h * group + g) * HD, HD)
            context_ref[:, cols] = context[g * tokens : (g + 1) * tokens]
    at = 0
    for distance in range(1, chips + 1):
        base = lax.rem(rank // 2 + distance, chips) * 2
        for core in (rank % 2, 1 - rank % 2):
            first = pl.multiple_of((base + core) * part, 8)
            out_ref[pl.ds(at, part), :] = context_ref[pl.ds(first, part), :]
            at += part
    project(out_ref, 0, w_ref, send_ref, keep_ref, part)


def project_kernel(part, first, context_ref, *refs):
    *weights, send_ref, keep_ref = refs
    start = 0
    for w_ref in weights:
        cols = pl.ds(start, w_ref.shape[1])
        send, keep = send_ref.at[:, cols], keep_ref.at[:, cols]
        project(context_ref, first, w_ref, send, keep, part)
        start += w_ref.shape[1]


def project_call(context, weights, part, first, rows):
    depth = context.shape[1]
    width = sum(weight.shape[1] for weight in weights)
    out = jax.ShapeDtypeStruct((rows // 2, width), jnp.bfloat16)
    return pl.pallas_call(
        functools.partial(project_kernel, part, first),
        out_shape=(out, out),
        in_specs=[VMEM] * (1 + len(weights)),
        out_specs=(VMEM, VMEM),
        cost_estimate=pl.CostEstimate(
            flops=2 * rows * depth * width,
            transcendentals=0,
            bytes_accessed=2 * depth * width,
        ),
        compiler_params=pltpu.CompilerParams(vmem_limit_bytes=PROJ * MIB),
        name="project_rest",
    )(context, *weights)


def finish_kernel(starts, kept_ref, received_ref, *refs):
    n = len(starts)
    *arrived, out_hbm = refs[: -n - 1]
    chunks, sems = refs[-n - 1 : -1], refs[-1]
    each = len(arrived) // n
    copies = []
    for i, start in enumerate(starts):
        cols = pl.ds(start, chunks[i].shape[1])
        total = kept_ref[:, cols].astype(jnp.float32)
        total = total + received_ref[:, cols].astype(jnp.float32)
        for ref in arrived[i * each : (i + 1) * each]:
            total = total + ref[...].astype(jnp.float32)
        chunks[i][...] = total.astype(jnp.bfloat16)
        copies.append(pltpu.make_async_copy(chunks[i], out_hbm.at[:, cols], sems.at[i]))
        copies[-1].start()
    for copy in copies:
        copy.wait()


def finish_call(kept, received, arrived, starts, out=None):
    flat = [block for blocks in arrived for block in blocks]
    n = len(starts)
    kernel = functools.partial(finish_kernel, starts)
    if out is not None:

        def kernel(kept_ref, received_ref, *refs):
            blocks, rest = refs[: len(flat)], refs[len(flat) + 1 :]
            finish_kernel(starts, kept_ref, received_ref, *blocks, *rest)

    return pl.pallas_call(
        kernel,
        out_shape=jax.ShapeDtypeStruct(kept.shape, kept.dtype),
        in_specs=[VMEM] * (2 + len(flat)) + [ANY] * (out is not None),
        out_specs=ANY,
        scratch_shapes=[pltpu.VMEM(blocks[0].shape, kept.dtype) for blocks in arrived]
        + [pltpu.SemaphoreType.DMA((n,))],
        input_output_aliases={} if out is None else {2 + len(flat): 0},
        cost_estimate=pl.CostEstimate(
            flops=4 * kept.size, transcendentals=0, bytes_accessed=4 * kept.size
        ),
        compiler_params=pltpu.CompilerParams(vmem_limit_bytes=4 * MIB),
        name="finish",
    )(kept, received, *flat, *([] if out is None else [out]))


def layer(query_rows, key_rows, value_rows, document_ids, output_weight):
    tokens = query_rows.shape[0]
    kv_local = key_rows.shape[1] // HD
    group = HEADS // KV
    width = query_rows.shape[1]
    model = output_weight.shape[1]
    seq, tp = lax.axis_size("seq"), lax.axis_size("tp")
    part = tokens // tp
    chips = tp // 2
    reach = min(12, seq // 2)
    depth = (reach + 1) // 2
    route = routes(seq, tp, depth)
    odd_row = (lax.axis_index("seq") // 2) % 2 == 1

    def send(x, name, step):
        return lax.ppermute(x, AXES, route[name, step])

    own = pl.pallas_call(
        join_kernel,
        out_shape=pltpu.VMEM((tokens, 2 * kv_local * HD), jnp.bfloat16),
        in_specs=[ANY, ANY],
        out_specs=VMEM,
        scratch_shapes=[pltpu.SemaphoreType.DMA((2,))],
        compiler_params=pltpu.CompilerParams(vmem_limit_bytes=2 * MIB),
        name="join",
    )(in_hbm(key_rows), in_hbm(value_rows))
    docs = document_ids.astype(jnp.float32).reshape(seq, tokens)
    cuts = [model * n // 32 for n in (0, *CUTS)]
    near = model * NEAR // 32
    weight = in_hbm(output_weight)
    first, *middle = load_call(weight, (0, cuts[1], near))
    *rest, third = load_call(weight, (near, *cuts[2:4]))
    weights = [[first], middle + rest, [third]]
    weights.append(load_call(weight, cuts[3:]))
    even, odd = send(own, "even", 1), send(own, "odd", 1)
    blocks = [own, send(own, "col", 0)]
    even, odd, docs = lax.optimization_barrier((even, odd, docs))
    for distance in range(1, depth + 1):
        blocks.append(jnp.where(odd_row, even, odd))
        if distance < depth:
            even, odd = (
                send(odd, "even", distance + 1),
                send(even, "odd", distance + 1),
            )
        blocks.append(send(blocks[-1], "col", distance))
    last_block = blocks.pop()
    count = len(blocks)

    stacked = group * tokens
    state = jax.ShapeDtypeStruct((kv_local * stacked, HD), jnp.float32)
    acc, top, total = pl.pallas_call(
        functools.partial(early_kernel, kv_local, group, count, 32),
        out_shape=(state, state, state),
        in_specs=[VMEM] * (2 + count),
        out_specs=(VMEM,) * 3,
        scratch_shapes=[
            pltpu.VMEM((tokens, count * tokens), jnp.float32),
            pltpu.VMEM((stacked, count * tokens), jnp.float32),
            pltpu.VMEM((stacked, count * tokens), jnp.bfloat16),
        ],
        cost_estimate=pl.CostEstimate(
            flops=4 * tokens * tokens * count * width,
            transcendentals=tokens * tokens * count * width // HD,
            bytes_accessed=4 * tokens * width,
        ),
        compiler_params=pltpu.CompilerParams(vmem_limit_bytes=EARLY * MIB),
        name="attend_early",
    )(query_rows, docs, *blocks)

    remote = (chips - 1) * part
    out = jax.ShapeDtypeStruct((remote, cuts[1]), jnp.bfloat16)
    context, sent, kept = pl.pallas_call(
        functools.partial(late_kernel, kv_local, group, part, depth),
        out_shape=(jax.ShapeDtypeStruct((tokens, width), jnp.bfloat16), out, out),
        in_specs=[VMEM] * 7,
        out_specs=(VMEM, VMEM, VMEM),
        scratch_shapes=[pltpu.VMEM((tokens, width), jnp.bfloat16)],
        cost_estimate=pl.CostEstimate(
            flops=4 * tokens * tokens * width + 2 * tokens * width * cuts[1],
            transcendentals=tokens * tokens * width // HD,
            bytes_accessed=4 * tokens * width + 2 * width * cuts[1],
        ),
        compiler_params=pltpu.CompilerParams(vmem_limit_bytes=LATE * MIB),
        name="attend_late",
    )(query_rows, docs, last_block, acc, top, total, first)

    arrived = []
    for i, weight in enumerate(weights):
        if i:
            sent, kept = project_call(context, weight, part, 0, 2 * remote)
        received = send(sent, "core", i)
        moved = kept.astype(jnp.float32) + received.astype(jnp.float32)
        moved = moved.astype(jnp.bfloat16)
        arrived.append([])
        for distance in range(1, chips):
            at = (distance - 1) * part
            block = lax.ppermute(
                moved[at : at + part], AXES, y_route(seq, tp, distance)
            )
            arrived[-1].append(block)
    every = [weight for weights_of in weights for weight in weights_of]
    sent, kept = project_call(context, every, part, 2 * remote, 2 * part)
    received = send(sent, "core", len(CUTS))
    out = finish_call(kept, received, arrived[:-1], cuts[:-2])
    return finish_call(kept, received, arrived[-1:], cuts[-2:-1], out)


def solution(mesh):
    in_specs = (P("seq", "tp"), P("seq", "tp"), P("seq", "tp"), P(), P("tp", None))
    out_specs = P(("seq", "tp"), None)
    return jax.shard_map(
        layer, mesh=mesh, in_specs=in_specs, out_specs=out_specs, check_vma=False
    )
```

```python
import functools

import jax
import jax.numpy as jnp
from jax import lax
from jax.experimental import pallas as pl
from jax.experimental.pallas import tpu as pltpu
from jax.sharding import PartitionSpec as P


HEADS = 32
KV = 8
HD = 128
AXES = ("seq", "tp")
LOG2E = 1.4426950408889634
SCALE = LOG2E / HD**0.5
VMEM = pl.BlockSpec(memory_space=pltpu.VMEM)
ANY = pl.BlockSpec(memory_space=pl.ANY)
MIB = 1 << 20
CUTS = (7, 17, 24, 32)
NEAR = 12
EARLY, LATE, PROJ = 24, 16, 8


def routes(seq, tp, depth):
    rows = seq // 2

    def flat(rule):
        pairs = []
        for s in range(seq):
            for t in range(tp):
                s2, t2 = rule(s, t)
                pairs.append((s * tp + t, s2 * tp + t2))
        return pairs

    def by_row(parity, step):
        def rule(s, t):
            row, col = divmod(s, 2)
            other = row + 1 if row % 2 == parity else row - 1
            if step - 1 <= min(row, other) and max(row, other) < rows:
                return other * 2 + col, t
            return s, t ^ 1

        return flat(rule)

    def by_col(step):
        return flat(lambda s, t: (s ^ 1, t) if s // 2 >= step else (s, t ^ 1))

    table = {("core", i): flat(lambda s, t: (s, t ^ 1)) for i in range(len(CUTS) + 1)}
    for step in range(depth + 1):
        table["col", step] = by_col(step)
        table["even", step] = by_row(0, step)
        table["odd", step] = by_row(1, step)
    return table


def y_route(seq, tp, distance):
    pairs = []
    for s in range(seq):
        for t in range(tp):
            pairs.append((s * tp + t, s * tp + (t + 2 * distance) % tp))
    return pairs


def join_kernel(k_ref, v_ref, out_ref, sems):
    copies = []
    for h in range(k_ref.shape[1] // HD):
        for i, ref in enumerate((k_ref, v_ref)):
            at = 2 * h + i
            into = out_ref.at[:, pl.ds(at * HD, HD)]
            source = ref.at[:, pl.ds(h * HD, HD)]
            copies.append(pltpu.make_async_copy(source, into, sems.at[at]))
    for copy in copies:
        copy.start()
    for copy in copies:
        copy.wait()


def load_kernel(start, w_hbm, *refs):
    *outs, sems = refs
    copies = []
    for i, out in enumerate(outs):
        width = out.shape[1]
        source = w_hbm.at[:, pl.ds(start, width)]
        copies.append(pltpu.make_async_copy(source, out, sems.at[i]))
        start += width
    for copy in copies:
        copy.start()
    for copy in copies:
        copy.wait()


def load_call(weight, cuts):
    depth = weight.shape[0]
    widths = [stop - start for start, stop in zip(cuts, cuts[1:])]
    return pl.pallas_call(
        functools.partial(load_kernel, cuts[0]),
        out_shape=[pltpu.VMEM((depth, width), weight.dtype) for width in widths],
        in_specs=[ANY],
        out_specs=[VMEM] * len(widths),
        scratch_shapes=[pltpu.SemaphoreType.DMA((len(widths),))],
        cost_estimate=pl.CostEstimate(
            flops=0,
            transcendentals=0,
            bytes_accessed=2 * depth * (cuts[-1] - cuts[0]),
        ),
        compiler_params=pltpu.CompilerParams(vmem_limit_bytes=MIB),
        name="load",
    )(weight)


def in_hbm(x):
    return pltpu.with_memory_space_constraint(x, pltpu.HBM)


def query_doc(docs_ref, me):
    docs = docs_ref[...]
    own = lax.broadcasted_iota(jnp.int32, (docs.shape[0], HD), 0) == me
    column = lax.dot_general(
        docs,
        own.astype(jnp.float32),
        (((0,), (0,)), ((), ())),
        precision=lax.Precision.HIGHEST,
        preferred_element_type=jnp.float32,
    )
    return column[:, :1]


def key_doc(docs_ref, block, me):
    row = docs_ref[pl.ds(jnp.maximum(block, 0), 1), :]
    return jnp.where((block >= 0) & (block <= me), row, -1.0)


def stack(q_ref, h, group):
    return jnp.concatenate(
        [q_ref[:, pl.ds((h * group + g) * HD, HD)] for g in range(group)], axis=0
    )


def scores_of(queries, keys):
    return lax.dot_general(
        queries, keys, (((1,), (1,)), ((), ())), preferred_element_type=jnp.float32
    )


def early_kernel(kv_local, group, count, step, *refs):
    q_ref, docs_ref = refs[:2]
    blocks = refs[2 : 2 + count]
    acc_ref, top_ref, sum_ref = refs[2 + count : 5 + count]
    bias_ref, s_ref, p_ref = refs[5 + count :]
    tokens = q_ref.shape[0]
    stacked = group * tokens
    me = lax.axis_index("seq")
    row, col = me // 2, me % 2
    docs = []
    for i in range(count):
        block = me - i if i % 2 == 0 else (row - i // 2) * 2 + 1 - col
        docs.append(key_doc(docs_ref, block, me))
    allowed = query_doc(docs_ref, me) == jnp.concatenate(docs, axis=1)
    key_at = lax.broadcasted_iota(jnp.int32, (tokens, count * tokens), 1)
    query_at = lax.broadcasted_iota(jnp.int32, (tokens, count * tokens), 0)
    allowed = allowed & ((key_at <= query_at) | (key_at >= tokens))
    bias_ref[...] = jnp.where(allowed, 0.0, -jnp.inf)
    for h in range(kv_local):
        cols = pl.ds(2 * h * HD, HD)
        keys = jnp.concatenate([b[:, cols] for b in blocks], axis=0)
        s_ref[...] = scores_of(stack(q_ref, h, group), keys)
        for r in range(0, stacked, step):
            at = pl.ds(r, step)
            into = pl.ds(h * stacked + r, step)
            scores = s_ref[at, :] * SCALE + bias_ref[pl.ds(r % tokens, step), :]
            top = jnp.max(scores, axis=-1, keepdims=True)
            weight = jnp.exp2(scores - top)
            total = jnp.sum(weight, axis=-1, keepdims=True)
            p_ref[at, :] = weight.astype(jnp.bfloat16)
            top_ref[into, :] = jnp.broadcast_to(top, (step, HD))
            sum_ref[into, :] = jnp.broadcast_to(total, (step, HD))
        cols = pl.ds((2 * h + 1) * HD, HD)
        values = jnp.concatenate([b[:, cols] for b in blocks], axis=0)
        acc_ref[pl.ds(h * stacked, stacked), :] = jnp.dot(
            p_ref[...], values, preferred_element_type=jnp.float32
        )


def project(context_ref, first, w_ref, send_ref, keep_ref, part, top=0, more_ref=None):
    step = 256
    count = keep_ref.shape[0] // part
    for c in range(0, w_ref.shape[1], step):
        at = pl.ds(c, step)
        rows = jnp.dot(
            context_ref[pl.ds(first, 2 * count * part), :],
            w_ref[pl.ds(top, context_ref.shape[1]), at],
            preferred_element_type=jnp.float32,
        )
        if more_ref is not None:
            rows = rows + more_ref[:, at]
        rows = rows.astype(jnp.bfloat16)
        for i in range(count):
            into = pl.ds(i * part, part)
            keep_ref[into, at] = rows[2 * i * part : (2 * i + 1) * part]
            send_ref[into, at] = rows[(2 * i + 1) * part : (2 * i + 2) * part]


def late_kernel(h, kv_local, group, part, depth, *refs):
    q_ref, docs_ref, block, acc_ref, top_ref, sum_ref, w_ref = refs[:7]
    context_ref, here_ref = refs[-2:]
    refs = refs[7:-2]
    tokens = q_ref.shape[0]
    stacked = group * tokens
    me, rank = lax.axis_index("seq"), lax.axis_index("tp")
    chips = lax.axis_size("tp") // 2
    far = (me // 2 - depth) * 2 + 1 - me % 2
    bias = jnp.where(
        query_doc(docs_ref, me) == key_doc(docs_ref, far, me), 0.0, -jnp.inf
    )
    keys, values = block[:, pl.ds(0, HD)], block[:, pl.ds(HD, HD)]
    scores = scores_of(stack(q_ref, h, group), keys)
    scores = scores * SCALE + jnp.concatenate([bias] * group, axis=0)
    at = pl.ds(h * stacked, stacked)
    old = top_ref[at, :]
    new = jnp.maximum(old[:, :1], jnp.max(scores, axis=-1, keepdims=True))
    weight = jnp.exp2(scores - new)
    rescale = jnp.exp2(old - new)
    total = sum_ref[at, :] * rescale + jnp.sum(weight, axis=-1, keepdims=True)
    added = jnp.dot(
        weight.astype(jnp.bfloat16), values, preferred_element_type=jnp.float32
    )
    context = (acc_ref[at, :] * rescale + added) / total
    context = context.astype(jnp.bfloat16)
    for g in range(group):
        rows = context[g * tokens : (g + 1) * tokens]
        context_ref[:, pl.ds(g * HD, HD)] = rows
    at = 0
    for distance in range(1, chips + 1):
        base = lax.rem(rank // 2 + distance, chips) * 2
        for core in (rank % 2, 1 - rank % 2):
            first = pl.multiple_of((base + core) * part, 8)
            here_ref[pl.ds(at, part), :] = context_ref[pl.ds(first, part), :]
            at += part
    depth_of = group * HD
    top = h * depth_of
    more_ref, before_ref = refs[:2] if h else (None, None)
    if h < kv_local - 1:
        part_ref, out_ref = refs[-2:]
        rows = part_ref.shape[0]
        step = 256
        for c in range(0, w_ref.shape[1], step):
            cols = pl.ds(c, step)
            product = jnp.dot(
                here_ref[pl.ds(0, rows), :],
                w_ref[pl.ds(top, depth_of), cols],
                preferred_element_type=jnp.float32,
            )
            part_ref[:, cols] = product if more_ref is None else product + more_ref[:, cols]
    else:
        send_ref, keep_ref, out_ref = refs[-3:]
        project(here_ref, 0, w_ref, send_ref, keep_ref, part, top, more_ref)
    out_ref[:, pl.ds(top, depth_of)] = here_ref[...]
    if h:
        out_ref[:, pl.ds(0, top)] = before_ref[...]


def project_kernel(part, first, context_ref, *refs):
    *weights, send_ref, keep_ref = refs
    start = 0
    for w_ref in weights:
        cols = pl.ds(start, w_ref.shape[1])
        send, keep = send_ref.at[:, cols], keep_ref.at[:, cols]
        project(context_ref, first, w_ref, send, keep, part)
        start += w_ref.shape[1]


def project_call(context, weights, part, first, rows):
    depth = context.shape[1]
    width = sum(weight.shape[1] for weight in weights)
    out = jax.ShapeDtypeStruct((rows // 2, width), jnp.bfloat16)
    return pl.pallas_call(
        functools.partial(project_kernel, part, first),
        out_shape=(out, out),
        in_specs=[VMEM] * (1 + len(weights)),
        out_specs=(VMEM, VMEM),
        cost_estimate=pl.CostEstimate(
            flops=2 * rows * depth * width,
            transcendentals=0,
            bytes_accessed=2 * depth * width,
        ),
        compiler_params=pltpu.CompilerParams(vmem_limit_bytes=PROJ * MIB),
        name="project_rest",
    )(context, *weights)


def finish_kernel(starts, kept_ref, received_ref, *refs):
    n = len(starts)
    *arrived, out_hbm = refs[: -n - 1]
    chunks, sems = refs[-n - 1 : -1], refs[-1]
    each = len(arrived) // n
    copies = []
    for i, start in enumerate(starts):
        cols = pl.ds(start, chunks[i].shape[1])
        total = kept_ref[:, cols].astype(jnp.float32)
        total = total + received_ref[:, cols].astype(jnp.float32)
        for ref in arrived[i * each : (i + 1) * each]:
            total = total + ref[...].astype(jnp.float32)
        chunks[i][...] = total.astype(jnp.bfloat16)
        copies.append(pltpu.make_async_copy(chunks[i], out_hbm.at[:, cols], sems.at[i]))
        copies[-1].start()
    for copy in copies:
        copy.wait()


def finish_call(kept, received, arrived, starts, out=None):
    flat = [block for blocks in arrived for block in blocks]
    n = len(starts)
    kernel = functools.partial(finish_kernel, starts)
    if out is not None:

        def kernel(kept_ref, received_ref, *refs):
            blocks, rest = refs[: len(flat)], refs[len(flat) + 1 :]
            finish_kernel(starts, kept_ref, received_ref, *blocks, *rest)

    return pl.pallas_call(
        kernel,
        out_shape=jax.ShapeDtypeStruct(kept.shape, kept.dtype),
        in_specs=[VMEM] * (2 + len(flat)) + [ANY] * (out is not None),
        out_specs=ANY,
        scratch_shapes=[pltpu.VMEM(blocks[0].shape, kept.dtype) for blocks in arrived]
        + [pltpu.SemaphoreType.DMA((n,))],
        input_output_aliases={} if out is None else {2 + len(flat): 0},
        cost_estimate=pl.CostEstimate(
            flops=4 * kept.size, transcendentals=0, bytes_accessed=4 * kept.size
        ),
        compiler_params=pltpu.CompilerParams(vmem_limit_bytes=4 * MIB),
        name="finish",
    )(kept, received, *flat, *([] if out is None else [out]))


def layer(query_rows, key_rows, value_rows, document_ids, output_weight):
    tokens = query_rows.shape[0]
    kv_local = key_rows.shape[1] // HD
    group = HEADS // KV
    width = query_rows.shape[1]
    model = output_weight.shape[1]
    seq, tp = lax.axis_size("seq"), lax.axis_size("tp")
    part = tokens // tp
    chips = tp // 2
    reach = min(12, seq // 2)
    depth = (reach + 1) // 2
    route = routes(seq, tp, depth)
    odd_row = (lax.axis_index("seq") // 2) % 2 == 1

    def send(x, name, step):
        return lax.ppermute(x, AXES, route[name, step])

    own = pl.pallas_call(
        join_kernel,
        out_shape=pltpu.VMEM((tokens, 2 * kv_local * HD), jnp.bfloat16),
        in_specs=[ANY, ANY],
        out_specs=VMEM,
        scratch_shapes=[pltpu.SemaphoreType.DMA((2 * kv_local,))],
        compiler_params=pltpu.CompilerParams(vmem_limit_bytes=2 * MIB),
        name="join",
    )(in_hbm(key_rows), in_hbm(value_rows))
    docs = document_ids.astype(jnp.float32).reshape(seq, tokens)
    cuts = [model * n // 32 for n in (0, *CUTS)]
    near = model * NEAR // 32
    weight = in_hbm(output_weight)
    first, *middle = load_call(weight, (0, cuts[1], near))
    *rest, third = load_call(weight, (near, *cuts[2:4]))
    weights = [[first], middle + rest, [third]]
    weights.append(load_call(weight, cuts[3:]))
    even, odd = send(own, "even", 1), send(own, "odd", 1)
    blocks = [own, send(own, "col", 0)]
    even, odd, docs = lax.optimization_barrier((even, odd, docs))
    for distance in range(1, depth + 1):
        blocks.append(jnp.where(odd_row, even, odd))
        if distance < depth:
            even, odd = (
                send(odd, "even", distance + 1),
                send(even, "odd", distance + 1),
            )
        if distance < depth:
            blocks.append(send(blocks[-1], "col", distance))
    last_blocks = []
    for h in range(kv_local):
        piece = blocks[-1][:, 2 * h * HD : 2 * (h + 1) * HD]
        last_blocks.append(lax.ppermute(piece, AXES, route["col", depth]))
    count = len(blocks)

    stacked = group * tokens
    state = jax.ShapeDtypeStruct((kv_local * stacked, HD), jnp.float32)
    early = pl.pallas_call(
        functools.partial(early_kernel, kv_local, group, count, 32),
        out_shape=(state, state, state),
        in_specs=[VMEM] * (2 + count),
        out_specs=(VMEM,) * 3,
        scratch_shapes=[
            pltpu.VMEM((tokens, count * tokens), jnp.float32),
            pltpu.VMEM((stacked, count * tokens), jnp.float32),
            pltpu.VMEM((stacked, count * tokens), jnp.bfloat16),
        ],
        cost_estimate=pl.CostEstimate(
            flops=4 * tokens * tokens * count * width,
            transcendentals=tokens * tokens * count * width // HD,
            bytes_accessed=4 * tokens * width,
        ),
        compiler_params=pltpu.CompilerParams(vmem_limit_bytes=EARLY * MIB),
        name="attend_early",
    )
    acc, top, total = early(query_rows, docs, *blocks)

    remote = (chips - 1) * part
    out = jax.ShapeDtypeStruct((remote, cuts[1]), jnp.bfloat16)
    share = group * HD
    so_far = ()
    for h, last_block in enumerate(last_blocks):
        context_shape = jax.ShapeDtypeStruct((tokens, (h + 1) * share), jnp.bfloat16)
        if h < kv_local - 1:
            product = jax.ShapeDtypeStruct((2 * remote, cuts[1]), jnp.float32)
            shapes = (product, context_shape)
        else:
            shapes = (out, out, context_shape)
        so_far = pl.pallas_call(
            functools.partial(late_kernel, h, kv_local, group, part, depth),
            out_shape=shapes,
            in_specs=[VMEM] * (7 + len(so_far)),
            out_specs=(VMEM,) * len(shapes),
            scratch_shapes=[pltpu.VMEM((tokens, share), jnp.bfloat16)] * 2,
            cost_estimate=pl.CostEstimate(
                flops=4 * tokens * tokens * share + 4 * remote * share * cuts[1],
                transcendentals=tokens * tokens * group,
                bytes_accessed=4 * tokens * share + 2 * share * cuts[1],
            ),
            compiler_params=pltpu.CompilerParams(vmem_limit_bytes=LATE * MIB),
            name="attend_late",
        )(query_rows, docs, last_block, acc, top, total, first, *so_far)
    sent, kept, context = so_far

    arrived = []
    for i, weight in enumerate(weights):
        if i:
            sent, kept = project_call(context, weight, part, 0, 2 * remote)
        received = send(sent, "core", i)
        moved = kept.astype(jnp.float32) + received.astype(jnp.float32)
        moved = moved.astype(jnp.bfloat16)
        arrived.append([])
        for distance in range(1, chips):
            at = (distance - 1) * part
            block = lax.ppermute(
                moved[at : at + part], AXES, y_route(seq, tp, distance)
            )
            arrived[-1].append(block)
    every = [weight for weights_of in weights for weight in weights_of]
    sent, kept = project_call(context, every, part, 2 * remote, 2 * part)
    received = send(sent, "core", len(CUTS))
    out = finish_call(kept, received, arrived[:-1], cuts[:-2])
    return finish_call(kept, received, arrived[-1:], cuts[-2:-1], out)


def solution(mesh):
    in_specs = (P("seq", "tp"), P("seq", "tp"), P("seq", "tp"), P(), P("tp", None))
    out_specs = P(("seq", "tp"), None)
    return jax.shard_map(
        layer, mesh=mesh, in_specs=in_specs, out_specs=out_specs, check_vma=False
    )
```

```python
import functools

import jax
import jax.numpy as jnp
from jax import lax
from jax.experimental import pallas as pl
from jax.experimental.pallas import tpu as pltpu
from jax.sharding import PartitionSpec as P


HEADS = 32
KV = 8
HD = 128
AXES = ("seq", "tp")
LOG2E = 1.4426950408889634
SCALE = LOG2E / HD**0.5
VMEM = pl.BlockSpec(memory_space=pltpu.VMEM)
ANY = pl.BlockSpec(memory_space=pl.ANY)
MIB = 1 << 20
CUTS = (7, 17, 24, 32)
NEAR = 12
EARLY, LATE, PROJ = 24, 16, 8


def routes(seq, tp, depth):
    rows = seq // 2

    def flat(rule):
        pairs = []
        for s in range(seq):
            for t in range(tp):
                s2, t2 = rule(s, t)
                pairs.append((s * tp + t, s2 * tp + t2))
        return pairs

    def by_row(parity, step):
        def rule(s, t):
            row, col = divmod(s, 2)
            other = row + 1 if row % 2 == parity else row - 1
            if step - 1 <= min(row, other) and max(row, other) < rows:
                return other * 2 + col, t
            return s, t ^ 1

        return flat(rule)

    def by_col(step):
        return flat(lambda s, t: (s ^ 1, t) if s // 2 >= step else (s, t ^ 1))

    table = {("core", i): flat(lambda s, t: (s, t ^ 1)) for i in range(len(CUTS) + 1)}
    for step in range(depth + 1):
        table["col", step] = by_col(step)
        table["even", step] = by_row(0, step)
        table["odd", step] = by_row(1, step)
    return table


def y_route(seq, tp, distance):
    pairs = []
    for s in range(seq):
        for t in range(tp):
            pairs.append((s * tp + t, s * tp + (t + 2 * distance) % tp))
    return pairs


def join_kernel(k_ref, v_ref, out_ref, sems):
    copies = []
    for h in range(k_ref.shape[1] // HD):
        for i, ref in enumerate((k_ref, v_ref)):
            at = 2 * h + i
            into = out_ref.at[:, pl.ds(at * HD, HD)]
            source = ref.at[:, pl.ds(h * HD, HD)]
            copies.append(pltpu.make_async_copy(source, into, sems.at[at]))
    for copy in copies:
        copy.start()
    for copy in copies:
        copy.wait()


def load_kernel(start, w_hbm, *refs):
    *outs, sems = refs
    copies = []
    for i, out in enumerate(outs):
        width = out.shape[1]
        source = w_hbm.at[:, pl.ds(start, width)]
        copies.append(pltpu.make_async_copy(source, out, sems.at[i]))
        start += width
    for copy in copies:
        copy.start()
    for copy in copies:
        copy.wait()


def load_call(weight, cuts):
    depth = weight.shape[0]
    widths = [stop - start for start, stop in zip(cuts, cuts[1:])]
    return pl.pallas_call(
        functools.partial(load_kernel, cuts[0]),
        out_shape=[pltpu.VMEM((depth, width), weight.dtype) for width in widths],
        in_specs=[ANY],
        out_specs=[VMEM] * len(widths),
        scratch_shapes=[pltpu.SemaphoreType.DMA((len(widths),))],
        cost_estimate=pl.CostEstimate(
            flops=0,
            transcendentals=0,
            bytes_accessed=2 * depth * (cuts[-1] - cuts[0]),
        ),
        compiler_params=pltpu.CompilerParams(vmem_limit_bytes=MIB),
        name="load",
    )(weight)


def in_hbm(x):
    return pltpu.with_memory_space_constraint(x, pltpu.HBM)


def query_doc(docs_ref, me):
    docs = docs_ref[...]
    own = lax.broadcasted_iota(jnp.int32, (docs.shape[0], HD), 0) == me
    column = lax.dot_general(
        docs,
        own.astype(jnp.float32),
        (((0,), (0,)), ((), ())),
        precision=lax.Precision.HIGHEST,
        preferred_element_type=jnp.float32,
    )
    return column[:, :1]


def key_doc(docs_ref, block, me):
    row = docs_ref[pl.ds(jnp.maximum(block, 0), 1), :]
    return jnp.where((block >= 0) & (block <= me), row, -1.0)


def stack(q_ref, h, group):
    return jnp.concatenate(
        [q_ref[:, pl.ds((h * group + g) * HD, HD)] for g in range(group)], axis=0
    )


def scores_of(queries, keys):
    return lax.dot_general(
        queries, keys, (((1,), (1,)), ((), ())), preferred_element_type=jnp.float32
    )


def with_ones(values):
    return jnp.concatenate([values, jnp.ones_like(values)], axis=1)


def early_kernel(kv_local, group, count, step, *refs):
    q_ref, docs_ref = refs[:2]
    blocks = refs[2 : 2 + count]
    acc_ref, top_ref, sum_ref = refs[2 + count : 5 + count]
    bias_ref, s_ref, p_ref = refs[5 + count :]
    tokens = q_ref.shape[0]
    me = lax.axis_index("seq")
    row, col = me // 2, me % 2
    docs = []
    for i in range(count):
        block = me - i if i % 2 == 0 else (row - i // 2) * 2 + 1 - col
        docs.append(key_doc(docs_ref, block, me))
    allowed = query_doc(docs_ref, me) == jnp.concatenate(docs, axis=1)
    key_at = lax.broadcasted_iota(jnp.int32, (tokens, count * tokens), 1)
    query_at = lax.broadcasted_iota(jnp.int32, (tokens, count * tokens), 0)
    allowed = allowed & ((key_at <= query_at) | (key_at >= tokens))
    bias_ref[...] = jnp.where(allowed, 0.0, -jnp.inf)
    keys, values = [], []
    for h in range(kv_local):
        at = pl.ds(2 * h * HD, HD)
        keys.append(jnp.concatenate([b[:, at] for b in blocks], axis=0))
        at = pl.ds((2 * h + 1) * HD, HD)
        values.append(with_ones(jnp.concatenate([b[:, at] for b in blocks], axis=0)))

    def score(head):
        s_ref[head] = scores_of(q_ref[:, pl.ds(head * HD, HD)], keys[head // group])

    def soften(head):
        for r in range(0, tokens, step):
            at = pl.ds(r, step)
            scores = s_ref[head, at, :] * SCALE + bias_ref[at, :]
            top = jnp.max(scores, axis=-1, keepdims=True)
            p_ref[head, at, :] = jnp.exp2(scores - top).astype(jnp.bfloat16)
            into = pl.ds(head * tokens + r, step)
            top_ref[into, :] = jnp.broadcast_to(top, (step, HD))

    def add_up(head):
        both = jnp.dot(
            p_ref[head], values[head // group], preferred_element_type=jnp.float32
        )
        into = pl.ds(head * tokens, tokens)
        acc_ref[into, :] = both[:, :HD]
        sum_ref[into, :] = both[:, HD:]

    heads = kv_local * group
    score(0)
    for head in range(heads):
        if head + 1 < heads:
            score(head + 1)
        soften(head)
        if head:
            add_up(head - 1)
    add_up(heads - 1)


def project(context_ref, first, w_ref, send_ref, keep_ref, part, top=0, more_ref=None):
    step = 256
    count = keep_ref.shape[0] // part
    for c in range(0, w_ref.shape[1], step):
        at = pl.ds(c, step)
        rows = jnp.dot(
            context_ref[pl.ds(first, 2 * count * part), :],
            w_ref[pl.ds(top, context_ref.shape[1]), at],
            preferred_element_type=jnp.float32,
        )
        if more_ref is not None:
            rows = rows + more_ref[:, at]
        rows = rows.astype(jnp.bfloat16)
        for i in range(count):
            into = pl.ds(i * part, part)
            keep_ref[into, at] = rows[2 * i * part : (2 * i + 1) * part]
            send_ref[into, at] = rows[(2 * i + 1) * part : (2 * i + 2) * part]


def late_kernel(h, kv_local, group, part, depth, *refs):
    q_ref, docs_ref, block, acc_ref, top_ref, sum_ref, w_ref = refs[:7]
    context_ref, here_ref = refs[-2:]
    refs = refs[7:-2]
    tokens = q_ref.shape[0]
    stacked = group * tokens
    me, rank = lax.axis_index("seq"), lax.axis_index("tp")
    chips = lax.axis_size("tp") // 2
    far = (me // 2 - depth) * 2 + 1 - me % 2
    bias = jnp.where(
        query_doc(docs_ref, me) == key_doc(docs_ref, far, me), 0.0, -jnp.inf
    )
    keys, values = block[:, pl.ds(0, HD)], block[:, pl.ds(HD, HD)]
    scores = scores_of(stack(q_ref, h, group), keys)
    scores = scores * SCALE + jnp.concatenate([bias] * group, axis=0)
    at = pl.ds(h * stacked, stacked)
    old = top_ref[at, :]
    new = jnp.maximum(old[:, :1], jnp.max(scores, axis=-1, keepdims=True))
    weight = jnp.exp2(scores - new)
    rescale = jnp.exp2(old - new)
    added = jnp.dot(
        weight.astype(jnp.bfloat16),
        with_ones(values),
        preferred_element_type=jnp.float32,
    )
    total = sum_ref[at, :] * rescale + added[:, HD:]
    context = (acc_ref[at, :] * rescale + added[:, :HD]) / total
    context = context.astype(jnp.bfloat16)
    for g in range(group):
        rows = context[g * tokens : (g + 1) * tokens]
        context_ref[:, pl.ds(g * HD, HD)] = rows
    at = 0
    for distance in range(1, chips + 1):
        base = lax.rem(rank // 2 + distance, chips) * 2
        for core in (rank % 2, 1 - rank % 2):
            first = pl.multiple_of((base + core) * part, 8)
            here_ref[pl.ds(at, part), :] = context_ref[pl.ds(first, part), :]
            at += part
    depth_of = group * HD
    top = h * depth_of
    more_ref, before_ref = refs[:2] if h else (None, None)
    if h < kv_local - 1:
        part_ref, out_ref = refs[-2:]
        rows = part_ref.shape[0]
        step = 256
        for c in range(0, w_ref.shape[1], step):
            cols = pl.ds(c, step)
            product = jnp.dot(
                here_ref[pl.ds(0, rows), :],
                w_ref[pl.ds(top, depth_of), cols],
                preferred_element_type=jnp.float32,
            )
            part_ref[:, cols] = product if more_ref is None else product + more_ref[:, cols]
    else:
        send_ref, keep_ref, out_ref = refs[-3:]
        project(here_ref, 0, w_ref, send_ref, keep_ref, part, top, more_ref)
    out_ref[:, pl.ds(top, depth_of)] = here_ref[...]
    if h:
        out_ref[:, pl.ds(0, top)] = before_ref[...]


def project_kernel(part, first, context_ref, *refs):
    *weights, send_ref, keep_ref = refs
    start = 0
    for w_ref in weights:
        cols = pl.ds(start, w_ref.shape[1])
        send, keep = send_ref.at[:, cols], keep_ref.at[:, cols]
        project(context_ref, first, w_ref, send, keep, part)
        start += w_ref.shape[1]


def project_call(context, weights, part, first, rows):
    depth = context.shape[1]
    width = sum(weight.shape[1] for weight in weights)
    out = jax.ShapeDtypeStruct((rows // 2, width), jnp.bfloat16)
    return pl.pallas_call(
        functools.partial(project_kernel, part, first),
        out_shape=(out, out),
        in_specs=[VMEM] * (1 + len(weights)),
        out_specs=(VMEM, VMEM),
        cost_estimate=pl.CostEstimate(
            flops=2 * rows * depth * width,
            transcendentals=0,
            bytes_accessed=2 * depth * width,
        ),
        compiler_params=pltpu.CompilerParams(vmem_limit_bytes=PROJ * MIB),
        name="project_rest",
    )(context, *weights)


def finish_kernel(starts, kept_ref, received_ref, *refs):
    n = len(starts)
    *arrived, out_hbm = refs[: -n - 1]
    chunks, sems = refs[-n - 1 : -1], refs[-1]
    each = len(arrived) // n
    copies = []
    for i, start in enumerate(starts):
        cols = pl.ds(start, chunks[i].shape[1])
        total = kept_ref[:, cols].astype(jnp.float32)
        total = total + received_ref[:, cols].astype(jnp.float32)
        for ref in arrived[i * each : (i + 1) * each]:
            total = total + ref[...].astype(jnp.float32)
        chunks[i][...] = total.astype(jnp.bfloat16)
        copies.append(pltpu.make_async_copy(chunks[i], out_hbm.at[:, cols], sems.at[i]))
        copies[-1].start()
    for copy in copies:
        copy.wait()


def finish_call(kept, received, arrived, starts, out=None):
    flat = [block for blocks in arrived for block in blocks]
    n = len(starts)
    kernel = functools.partial(finish_kernel, starts)
    if out is not None:

        def kernel(kept_ref, received_ref, *refs):
            blocks, rest = refs[: len(flat)], refs[len(flat) + 1 :]
            finish_kernel(starts, kept_ref, received_ref, *blocks, *rest)

    return pl.pallas_call(
        kernel,
        out_shape=jax.ShapeDtypeStruct(kept.shape, kept.dtype),
        in_specs=[VMEM] * (2 + len(flat)) + [ANY] * (out is not None),
        out_specs=ANY,
        scratch_shapes=[pltpu.VMEM(blocks[0].shape, kept.dtype) for blocks in arrived]
        + [pltpu.SemaphoreType.DMA((n,))],
        input_output_aliases={} if out is None else {2 + len(flat): 0},
        cost_estimate=pl.CostEstimate(
            flops=4 * kept.size, transcendentals=0, bytes_accessed=4 * kept.size
        ),
        compiler_params=pltpu.CompilerParams(vmem_limit_bytes=4 * MIB),
        name="finish",
    )(kept, received, *flat, *([] if out is None else [out]))


def layer(query_rows, key_rows, value_rows, document_ids, output_weight):
    tokens = query_rows.shape[0]
    kv_local = key_rows.shape[1] // HD
    group = HEADS // KV
    width = query_rows.shape[1]
    model = output_weight.shape[1]
    seq, tp = lax.axis_size("seq"), lax.axis_size("tp")
    part = tokens // tp
    chips = tp // 2
    reach = min(12, seq // 2)
    depth = (reach + 1) // 2
    route = routes(seq, tp, depth)
    odd_row = (lax.axis_index("seq") // 2) % 2 == 1

    def send(x, name, step):
        return lax.ppermute(x, AXES, route[name, step])

    own = pl.pallas_call(
        join_kernel,
        out_shape=pltpu.VMEM((tokens, 2 * kv_local * HD), jnp.bfloat16),
        in_specs=[ANY, ANY],
        out_specs=VMEM,
        scratch_shapes=[pltpu.SemaphoreType.DMA((2 * kv_local,))],
        compiler_params=pltpu.CompilerParams(vmem_limit_bytes=2 * MIB),
        name="join",
    )(in_hbm(key_rows), in_hbm(value_rows))
    docs = document_ids.astype(jnp.float32).reshape(seq, tokens)
    cuts = [model * n // 32 for n in (0, *CUTS)]
    near = model * NEAR // 32
    weight = in_hbm(output_weight)
    first, *middle = load_call(weight, (0, cuts[1], near))
    *rest, third = load_call(weight, (near, *cuts[2:4]))
    weights = [[first], middle + rest, [third]]
    weights.append(load_call(weight, cuts[3:]))
    even, odd = send(own, "even", 1), send(own, "odd", 1)
    blocks = [own, send(own, "col", 0)]
    even, odd, docs = lax.optimization_barrier((even, odd, docs))
    for distance in range(1, depth + 1):
        blocks.append(jnp.where(odd_row, even, odd))
        if distance < depth:
            even, odd = (
                send(odd, "even", distance + 1),
                send(even, "odd", distance + 1),
            )
        if distance < depth:
            blocks.append(send(blocks[-1], "col", distance))
    last_blocks = []
    for h in range(kv_local):
        piece = blocks[-1][:, 2 * h * HD : 2 * (h + 1) * HD]
        last_blocks.append(lax.ppermute(piece, AXES, route["col", depth]))
    count = len(blocks)

    stacked = group * tokens
    state = jax.ShapeDtypeStruct((kv_local * stacked, HD), jnp.float32)
    early = pl.pallas_call(
        functools.partial(early_kernel, kv_local, group, count, 64),
        out_shape=(state, state, state),
        in_specs=[VMEM] * (2 + count),
        out_specs=(VMEM,) * 3,
        scratch_shapes=[
            pltpu.VMEM((tokens, count * tokens), jnp.float32),
            pltpu.VMEM((kv_local * group, tokens, count * tokens), jnp.float32),
            pltpu.VMEM((kv_local * group, tokens, count * tokens), jnp.bfloat16),
        ],
        cost_estimate=pl.CostEstimate(
            flops=4 * tokens * tokens * count * width,
            transcendentals=tokens * tokens * count * width // HD,
            bytes_accessed=4 * tokens * width,
        ),
        compiler_params=pltpu.CompilerParams(vmem_limit_bytes=EARLY * MIB),
        name="attend_early",
    )
    acc, top, total = early(query_rows, docs, *blocks)

    remote = (chips - 1) * part
    out = jax.ShapeDtypeStruct((remote, cuts[1]), jnp.bfloat16)
    share = group * HD
    so_far = ()
    for h, last_block in enumerate(last_blocks):
        context_shape = jax.ShapeDtypeStruct((tokens, (h + 1) * share), jnp.bfloat16)
        if h < kv_local - 1:
            product = jax.ShapeDtypeStruct((2 * remote, cuts[1]), jnp.float32)
            shapes = (product, context_shape)
        else:
            shapes = (out, out, context_shape)
        so_far = pl.pallas_call(
            functools.partial(late_kernel, h, kv_local, group, part, depth),
            out_shape=shapes,
            in_specs=[VMEM] * (7 + len(so_far)),
            out_specs=(VMEM,) * len(shapes),
            scratch_shapes=[pltpu.VMEM((tokens, share), jnp.bfloat16)] * 2,
            cost_estimate=pl.CostEstimate(
                flops=4 * tokens * tokens * share + 4 * remote * share * cuts[1],
                transcendentals=tokens * tokens * group,
                bytes_accessed=4 * tokens * share + 2 * share * cuts[1],
            ),
            compiler_params=pltpu.CompilerParams(vmem_limit_bytes=LATE * MIB),
            name="attend_late",
        )(query_rows, docs, last_block, acc, top, total, first, *so_far)
    sent, kept, context = so_far

    arrived = []
    for i, weight in enumerate(weights):
        if i:
            sent, kept = project_call(context, weight, part, 0, 2 * remote)
        received = send(sent, "core", i)
        moved = kept.astype(jnp.float32) + received.astype(jnp.float32)
        moved = moved.astype(jnp.bfloat16)
        arrived.append([])
        for distance in range(1, chips):
            at = (distance - 1) * part
            block = lax.ppermute(
                moved[at : at + part], AXES, y_route(seq, tp, distance)
            )
            arrived[-1].append(block)
    every = [weight for weights_of in weights for weight in weights_of]
    sent, kept = project_call(context, every, part, 2 * remote, 2 * part)
    received = send(sent, "core", len(CUTS))
    out = finish_call(kept, received, arrived[:-1], cuts[:-2])
    return finish_call(kept, received, arrived[-1:], cuts[-2:-1], out)


def solution(mesh):
    in_specs = (P("seq", "tp"), P("seq", "tp"), P("seq", "tp"), P(), P("tp", None))
    out_specs = P(("seq", "tp"), None)
    return jax.shard_map(
        layer, mesh=mesh, in_specs=in_specs, out_specs=out_specs, check_vma=False
    )
```

```python
import functools

import jax
import jax.numpy as jnp
from jax import lax
from jax.experimental import pallas as pl
from jax.experimental.pallas import tpu as pltpu
from jax.sharding import PartitionSpec as P


HEADS = 32
KV = 8
HD = 128
AXES = ("seq", "tp")
LOG2E = 1.4426950408889634
SCALE = LOG2E / HD**0.5
VMEM = pl.BlockSpec(memory_space=pltpu.VMEM)
ANY = pl.BlockSpec(memory_space=pl.ANY)
MIB = 1 << 20
CUTS = (5, 15, 25, 32)
NEAR = 12
EARLY, LATE, PROJ = 24, 16, 8


def routes(seq, tp, depth):
    rows = seq // 2

    def flat(rule):
        pairs = []
        for s in range(seq):
            for t in range(tp):
                s2, t2 = rule(s, t)
                pairs.append((s * tp + t, s2 * tp + t2))
        return pairs

    def by_row(parity, step):
        def rule(s, t):
            row, col = divmod(s, 2)
            other = row + 1 if row % 2 == parity else row - 1
            if step - 1 <= min(row, other) and max(row, other) < rows:
                return other * 2 + col, t
            return s, t ^ 1

        return flat(rule)

    def by_col(step):
        return flat(lambda s, t: (s ^ 1, t) if s // 2 >= step else (s, t ^ 1))

    table = {("core", i): flat(lambda s, t: (s, t ^ 1)) for i in range(len(CUTS) + 1)}
    for step in range(depth + 1):
        table["col", step] = by_col(step)
        table["even", step] = by_row(0, step)
        table["odd", step] = by_row(1, step)
    return table


def y_route(seq, tp, distance):
    pairs = []
    for s in range(seq):
        for t in range(tp):
            pairs.append((s * tp + t, s * tp + (t + 2 * distance) % tp))
    return pairs


def join_kernel(k_ref, v_ref, out_ref, sems):
    copies = []
    for h in range(k_ref.shape[1] // HD):
        for i, ref in enumerate((k_ref, v_ref)):
            at = 2 * h + i
            into = out_ref.at[:, pl.ds(at * HD, HD)]
            source = ref.at[:, pl.ds(h * HD, HD)]
            copies.append(pltpu.make_async_copy(source, into, sems.at[at]))
    for copy in copies:
        copy.start()
    for copy in copies:
        copy.wait()


def load_kernel(start, w_hbm, *refs):
    *outs, sems = refs
    copies = []
    for i, out in enumerate(outs):
        width = out.shape[1]
        source = w_hbm.at[:, pl.ds(start, width)]
        copies.append(pltpu.make_async_copy(source, out, sems.at[i]))
        start += width
    for copy in copies:
        copy.start()
    for copy in copies:
        copy.wait()


def load_call(weight, cuts):
    depth = weight.shape[0]
    widths = [stop - start for start, stop in zip(cuts, cuts[1:])]
    return pl.pallas_call(
        functools.partial(load_kernel, cuts[0]),
        out_shape=[pltpu.VMEM((depth, width), weight.dtype) for width in widths],
        in_specs=[ANY],
        out_specs=[VMEM] * len(widths),
        scratch_shapes=[pltpu.SemaphoreType.DMA((len(widths),))],
        cost_estimate=pl.CostEstimate(
            flops=0,
            transcendentals=0,
            bytes_accessed=2 * depth * (cuts[-1] - cuts[0]),
        ),
        compiler_params=pltpu.CompilerParams(vmem_limit_bytes=MIB),
        name="load",
    )(weight)


def in_hbm(x):
    return pltpu.with_memory_space_constraint(x, pltpu.HBM)


def query_doc(docs_ref, me):
    docs = docs_ref[...]
    own = lax.broadcasted_iota(jnp.int32, (docs.shape[0], HD), 0) == me
    column = lax.dot_general(
        docs,
        own.astype(jnp.float32),
        (((0,), (0,)), ((), ())),
        precision=lax.Precision.HIGHEST,
        preferred_element_type=jnp.float32,
    )
    return column[:, :1]


def key_doc(docs_ref, block, me):
    row = docs_ref[pl.ds(jnp.maximum(block, 0), 1), :]
    return jnp.where((block >= 0) & (block <= me), row, -1.0)


def scores_of(queries, keys):
    return lax.dot_general(
        queries, keys, (((1,), (1,)), ((), ())), preferred_element_type=jnp.float32
    )


def with_ones(values):
    return jnp.concatenate([values, jnp.ones_like(values)], axis=1)


def early_kernel(kv_local, group, count, step, *refs):
    q_ref, docs_ref = refs[:2]
    blocks = refs[2 : 2 + count]
    acc_ref, top_ref, sum_ref = refs[2 + count : 5 + count]
    bias_ref, s_ref, p_ref = refs[5 + count :]
    tokens = q_ref.shape[0]
    me = lax.axis_index("seq")
    row, col = me // 2, me % 2
    docs = []
    for i in range(count):
        block = me - i if i % 2 == 0 else (row - i // 2) * 2 + 1 - col
        docs.append(key_doc(docs_ref, block, me))
    allowed = query_doc(docs_ref, me) == jnp.concatenate(docs, axis=1)
    key_at = lax.broadcasted_iota(jnp.int32, (tokens, count * tokens), 1)
    query_at = lax.broadcasted_iota(jnp.int32, (tokens, count * tokens), 0)
    allowed = allowed & ((key_at <= query_at) | (key_at >= tokens))
    bias_ref[...] = jnp.where(allowed, 0.0, -jnp.inf)
    keys, values = [], []
    for h in range(kv_local):
        at = pl.ds(2 * h * HD, HD)
        keys.append(jnp.concatenate([b[:, at] for b in blocks], axis=0))
        at = pl.ds((2 * h + 1) * HD, HD)
        values.append(with_ones(jnp.concatenate([b[:, at] for b in blocks], axis=0)))

    def score(head):
        s_ref[head] = scores_of(q_ref[:, pl.ds(head * HD, HD)], keys[head // group])

    def soften(head):
        for r in range(0, tokens, step):
            at = pl.ds(r, step)
            scores = s_ref[head, at, :] * SCALE + bias_ref[at, :]
            top = jnp.max(scores, axis=-1, keepdims=True)
            p_ref[head, at, :] = jnp.exp2(scores - top).astype(jnp.bfloat16)
            into = pl.ds(head * tokens + r, step)
            top_ref[into, :] = jnp.broadcast_to(top, (step, HD))

    def add_up(head):
        both = jnp.dot(
            p_ref[head], values[head // group], preferred_element_type=jnp.float32
        )
        into = pl.ds(head * tokens, tokens)
        acc_ref[into, :] = both[:, :HD]
        sum_ref[into, :] = both[:, HD:]

    heads = kv_local * group
    score(0)
    for head in range(heads):
        if head + 1 < heads:
            score(head + 1)
        soften(head)
        if head:
            add_up(head - 1)
    add_up(heads - 1)


def project(context_ref, first, w_ref, send_ref, keep_ref, part, top=0, more_ref=None):
    step = 256
    count = keep_ref.shape[0] // part
    for c in range(0, w_ref.shape[1], step):
        at = pl.ds(c, step)
        rows = jnp.dot(
            context_ref[pl.ds(first, 2 * count * part), :],
            w_ref[pl.ds(top, context_ref.shape[1]), at],
            preferred_element_type=jnp.float32,
        )
        if more_ref is not None:
            rows = rows + more_ref[:, at]
        rows = rows.astype(jnp.bfloat16)
        for i in range(count):
            into = pl.ds(i * part, part)
            keep_ref[into, at] = rows[2 * i * part : (2 * i + 1) * part]
            send_ref[into, at] = rows[(2 * i + 1) * part : (2 * i + 2) * part]


def late_kernel(h, kv_local, group, part, depth, step, *refs):
    q_ref, docs_ref, block, acc_ref, top_ref, sum_ref, w_ref = refs[:7]
    context_ref, here_ref, bias_ref, s_ref, p_ref, rescale_ref = refs[-6:]
    refs = refs[7:-6]
    tokens = q_ref.shape[0]
    me, rank = lax.axis_index("seq"), lax.axis_index("tp")
    chips = lax.axis_size("tp") // 2
    far = (me // 2 - depth) * 2 + 1 - me % 2
    bias_ref[...] = jnp.where(
        query_doc(docs_ref, me) == key_doc(docs_ref, far, me), 0.0, -jnp.inf
    )
    keys, values = block[:, pl.ds(0, HD)], with_ones(block[:, pl.ds(HD, HD)])

    def score(g):
        cols = pl.ds((h * group + g) * HD, HD)
        s_ref[g] = scores_of(q_ref[:, cols], keys)

    def soften(g):
        for r in range(0, tokens, step):
            at = pl.ds(r, step)
            scores = s_ref[g, at, :] * SCALE + bias_ref[at, :]
            old = top_ref[pl.ds((h * group + g) * tokens + r, step), :]
            new = jnp.maximum(old, jnp.max(scores, axis=-1, keepdims=True))
            p_ref[g, at, :] = jnp.exp2(scores - new[:, :1]).astype(jnp.bfloat16)
            rescale_ref[g, at, :] = jnp.exp2(old - new)

    def add_up(g):
        at = pl.ds((h * group + g) * tokens, tokens)
        added = jnp.dot(p_ref[g], values, preferred_element_type=jnp.float32)
        rescale = rescale_ref[g]
        total = sum_ref[at, :] * rescale + added[:, HD:]
        context = (acc_ref[at, :] * rescale + added[:, :HD]) / total
        context_ref[:, pl.ds(g * HD, HD)] = context.astype(jnp.bfloat16)

    score(0)
    for g in range(group):
        if g + 1 < group:
            score(g + 1)
        soften(g)
        if g:
            add_up(g - 1)
    add_up(group - 1)
    at = 0
    for distance in range(1, chips + 1):
        base = lax.rem(rank // 2 + distance, chips) * 2
        for core in (rank % 2, 1 - rank % 2):
            first = pl.multiple_of((base + core) * part, 8)
            here_ref[pl.ds(at, part), :] = context_ref[pl.ds(first, part), :]
            at += part
    depth_of = group * HD
    top = h * depth_of
    more_ref, before_ref = refs[:2] if h else (None, None)
    if h < kv_local - 1:
        part_ref, out_ref = refs[-2:]
        rows = part_ref.shape[0]
        step = 256
        for c in range(0, w_ref.shape[1], step):
            cols = pl.ds(c, step)
            product = jnp.dot(
                here_ref[pl.ds(0, rows), :],
                w_ref[pl.ds(top, depth_of), cols],
                preferred_element_type=jnp.float32,
            )
            part_ref[:, cols] = product if more_ref is None else product + more_ref[:, cols]
    else:
        send_ref, keep_ref, out_ref = refs[-3:]
        project(here_ref, 0, w_ref, send_ref, keep_ref, part, top, more_ref)
    out_ref[:, pl.ds(top, depth_of)] = here_ref[...]
    if h:
        out_ref[:, pl.ds(0, top)] = before_ref[...]


def project_kernel(part, first, context_ref, *refs):
    *weights, send_ref, keep_ref = refs
    start = 0
    for w_ref in weights:
        cols = pl.ds(start, w_ref.shape[1])
        send, keep = send_ref.at[:, cols], keep_ref.at[:, cols]
        project(context_ref, first, w_ref, send, keep, part)
        start += w_ref.shape[1]


def project_call(context, weights, part, first, rows):
    depth = context.shape[1]
    width = sum(weight.shape[1] for weight in weights)
    out = jax.ShapeDtypeStruct((rows // 2, width), jnp.bfloat16)
    return pl.pallas_call(
        functools.partial(project_kernel, part, first),
        out_shape=(out, out),
        in_specs=[VMEM] * (1 + len(weights)),
        out_specs=(VMEM, VMEM),
        cost_estimate=pl.CostEstimate(
            flops=2 * rows * depth * width,
            transcendentals=0,
            bytes_accessed=2 * depth * width,
        ),
        compiler_params=pltpu.CompilerParams(vmem_limit_bytes=PROJ * MIB),
        name="project_rest",
    )(context, *weights)


def finish_kernel(starts, kept_ref, received_ref, *refs):
    n = len(starts)
    *arrived, out_hbm = refs[: -n - 1]
    chunks, sems = refs[-n - 1 : -1], refs[-1]
    each = len(arrived) // n
    copies = []
    for i, start in enumerate(starts):
        cols = pl.ds(start, chunks[i].shape[1])
        total = kept_ref[:, cols].astype(jnp.float32)
        total = total + received_ref[:, cols].astype(jnp.float32)
        for ref in arrived[i * each : (i + 1) * each]:
            total = total + ref[...].astype(jnp.float32)
        chunks[i][...] = total.astype(jnp.bfloat16)
        copies.append(pltpu.make_async_copy(chunks[i], out_hbm.at[:, cols], sems.at[i]))
        copies[-1].start()
    for copy in copies:
        copy.wait()


def finish_call(kept, received, arrived, starts, out=None):
    flat = [block for blocks in arrived for block in blocks]
    n = len(starts)
    kernel = functools.partial(finish_kernel, starts)
    if out is not None:

        def kernel(kept_ref, received_ref, *refs):
            blocks, rest = refs[: len(flat)], refs[len(flat) + 1 :]
            finish_kernel(starts, kept_ref, received_ref, *blocks, *rest)

    return pl.pallas_call(
        kernel,
        out_shape=jax.ShapeDtypeStruct(kept.shape, kept.dtype),
        in_specs=[VMEM] * (2 + len(flat)) + [ANY] * (out is not None),
        out_specs=ANY,
        scratch_shapes=[pltpu.VMEM(blocks[0].shape, kept.dtype) for blocks in arrived]
        + [pltpu.SemaphoreType.DMA((n,))],
        input_output_aliases={} if out is None else {2 + len(flat): 0},
        cost_estimate=pl.CostEstimate(
            flops=4 * kept.size, transcendentals=0, bytes_accessed=4 * kept.size
        ),
        compiler_params=pltpu.CompilerParams(vmem_limit_bytes=4 * MIB),
        name="finish",
    )(kept, received, *flat, *([] if out is None else [out]))


def layer(query_rows, key_rows, value_rows, document_ids, output_weight):
    tokens = query_rows.shape[0]
    kv_local = key_rows.shape[1] // HD
    group = HEADS // KV
    width = query_rows.shape[1]
    model = output_weight.shape[1]
    seq, tp = lax.axis_size("seq"), lax.axis_size("tp")
    part = tokens // tp
    chips = tp // 2
    reach = min(12, seq // 2)
    depth = (reach + 1) // 2
    route = routes(seq, tp, depth)
    odd_row = (lax.axis_index("seq") // 2) % 2 == 1

    def send(x, name, step):
        return lax.ppermute(x, AXES, route[name, step])

    own = pl.pallas_call(
        join_kernel,
        out_shape=pltpu.VMEM((tokens, 2 * kv_local * HD), jnp.bfloat16),
        in_specs=[ANY, ANY],
        out_specs=VMEM,
        scratch_shapes=[pltpu.SemaphoreType.DMA((2 * kv_local,))],
        compiler_params=pltpu.CompilerParams(vmem_limit_bytes=2 * MIB),
        name="join",
    )(in_hbm(key_rows), in_hbm(value_rows))
    docs = document_ids.astype(jnp.float32).reshape(seq, tokens)
    cuts = [model * n // 32 for n in (0, *CUTS)]
    near = model * NEAR // 32
    weight = in_hbm(output_weight)
    first, *middle = load_call(weight, (0, cuts[1], near))
    *rest, third = load_call(weight, (near, *cuts[2:4]))
    weights = [[first], middle + rest, [third]]
    weights.append(load_call(weight, cuts[3:]))
    even, odd = send(own, "even", 1), send(own, "odd", 1)
    blocks = [own, send(own, "col", 0)]
    even, odd, docs = lax.optimization_barrier((even, odd, docs))
    for distance in range(1, depth + 1):
        blocks.append(jnp.where(odd_row, even, odd))
        if distance < depth:
            even, odd = (
                send(odd, "even", distance + 1),
                send(even, "odd", distance + 1),
            )
        if distance < depth:
            blocks.append(send(blocks[-1], "col", distance))
    last_blocks = []
    for h in range(kv_local):
        piece = blocks[-1][:, 2 * h * HD : 2 * (h + 1) * HD]
        last_blocks.append(lax.ppermute(piece, AXES, route["col", depth]))
    count = len(blocks)

    stacked = group * tokens
    state = jax.ShapeDtypeStruct((kv_local * stacked, HD), jnp.float32)
    early = pl.pallas_call(
        functools.partial(early_kernel, kv_local, group, count, 64),
        out_shape=(state, state, state),
        in_specs=[VMEM] * (2 + count),
        out_specs=(VMEM,) * 3,
        scratch_shapes=[
            pltpu.VMEM((tokens, count * tokens), jnp.float32),
            pltpu.VMEM((kv_local * group, tokens, count * tokens), jnp.float32),
            pltpu.VMEM((kv_local * group, tokens, count * tokens), jnp.bfloat16),
        ],
        cost_estimate=pl.CostEstimate(
            flops=4 * tokens * tokens * count * width,
            transcendentals=tokens * tokens * count * width // HD,
            bytes_accessed=4 * tokens * width,
        ),
        compiler_params=pltpu.CompilerParams(vmem_limit_bytes=EARLY * MIB),
        name="attend_early",
    )
    acc, top, total = early(query_rows, docs, *blocks)

    remote = (chips - 1) * part
    out = jax.ShapeDtypeStruct((remote, cuts[1]), jnp.bfloat16)
    share = group * HD
    so_far = ()
    for h, last_block in enumerate(last_blocks):
        context_shape = jax.ShapeDtypeStruct((tokens, (h + 1) * share), jnp.bfloat16)
        if h < kv_local - 1:
            product = jax.ShapeDtypeStruct((2 * remote, cuts[1]), jnp.float32)
            shapes = (product, context_shape)
        else:
            shapes = (out, out, context_shape)
        so_far = pl.pallas_call(
            functools.partial(late_kernel, h, kv_local, group, part, depth, 64),
            out_shape=shapes,
            in_specs=[VMEM] * (7 + len(so_far)),
            out_specs=(VMEM,) * len(shapes),
            scratch_shapes=[
                pltpu.VMEM((tokens, share), jnp.bfloat16),
                pltpu.VMEM((tokens, share), jnp.bfloat16),
                pltpu.VMEM((tokens, tokens), jnp.float32),
                pltpu.VMEM((group, tokens, tokens), jnp.float32),
                pltpu.VMEM((group, tokens, tokens), jnp.bfloat16),
                pltpu.VMEM((group, tokens, HD), jnp.float32),
            ],
            cost_estimate=pl.CostEstimate(
                flops=4 * tokens * tokens * share + 4 * remote * share * cuts[1],
                transcendentals=tokens * tokens * group,
                bytes_accessed=4 * tokens * share + 2 * share * cuts[1],
            ),
            compiler_params=pltpu.CompilerParams(vmem_limit_bytes=LATE * MIB),
            name="attend_late",
        )(query_rows, docs, last_block, acc, top, total, first, *so_far)
    sent, kept, context = so_far

    arrived = []
    for i, weight in enumerate(weights):
        if i:
            sent, kept = project_call(context, weight, part, 0, 2 * remote)
        received = send(sent, "core", i)
        moved = kept.astype(jnp.float32) + received.astype(jnp.float32)
        moved = moved.astype(jnp.bfloat16)
        arrived.append([])
        for distance in range(1, chips):
            at = (distance - 1) * part
            block = lax.ppermute(
                moved[at : at + part], AXES, y_route(seq, tp, distance)
            )
            arrived[-1].append(block)
    every = [weight for weights_of in weights for weight in weights_of]
    sent, kept = project_call(context, every, part, 2 * remote, 2 * part)
    received = send(sent, "core", len(CUTS))
    out = finish_call(kept, received, arrived[:-1], cuts[:-2])
    return finish_call(kept, received, arrived[-1:], cuts[-2:-1], out)


def solution(mesh):
    in_specs = (P("seq", "tp"), P("seq", "tp"), P("seq", "tp"), P(), P("tp", None))
    out_specs = P(("seq", "tp"), None)
    return jax.shard_map(
        layer, mesh=mesh, in_specs=in_specs, out_specs=out_specs, check_vma=False
    )
```

```python
import functools

import jax
import jax.numpy as jnp
from jax import lax
from jax.experimental import pallas as pl
from jax.experimental.pallas import tpu as pltpu
from jax.sharding import PartitionSpec as P


HEADS = 32
KV = 8
HD = 128
AXES = ("seq", "tp")
LOG2E = 1.4426950408889634
SCALE = LOG2E / HD**0.5
VMEM = pl.BlockSpec(memory_space=pltpu.VMEM)
ANY = pl.BlockSpec(memory_space=pl.ANY)
MIB = 1 << 20
CUTS = (5, 15, 25, 32)
NEAR = 12
EARLY, LATE, PROJ = 24, 16, 8


def routes(seq, tp, depth):
    rows = seq // 2

    def flat(rule):
        pairs = []
        for s in range(seq):
            for t in range(tp):
                s2, t2 = rule(s, t)
                pairs.append((s * tp + t, s2 * tp + t2))
        return pairs

    def by_row(parity, step):
        def rule(s, t):
            row, col = divmod(s, 2)
            other = row + 1 if row % 2 == parity else row - 1
            if step - 1 <= min(row, other) and max(row, other) < rows:
                return other * 2 + col, t
            return s, t ^ 1

        return flat(rule)

    def by_col(step):
        return flat(lambda s, t: (s ^ 1, t) if s // 2 >= step else (s, t ^ 1))

    table = {("core", i): flat(lambda s, t: (s, t ^ 1)) for i in range(len(CUTS) + 1)}
    for step in range(depth + 1):
        table["col", step] = by_col(step)
        table["even", step] = by_row(0, step)
        table["odd", step] = by_row(1, step)
    return table


def y_route(seq, tp, distance):
    pairs = []
    for s in range(seq):
        for t in range(tp):
            pairs.append((s * tp + t, s * tp + (t + 2 * distance) % tp))
    return pairs


def join_kernel(k_ref, v_ref, out_ref, sems):
    copies = []
    for h in range(k_ref.shape[1] // HD):
        for i, ref in enumerate((k_ref, v_ref)):
            at = 2 * h + i
            into = out_ref.at[:, pl.ds(at * HD, HD)]
            source = ref.at[:, pl.ds(h * HD, HD)]
            copies.append(pltpu.make_async_copy(source, into, sems.at[at]))
    for copy in copies:
        copy.start()
    for copy in copies:
        copy.wait()


def load_kernel(start, w_hbm, *refs):
    *outs, sems = refs
    copies = []
    for i, out in enumerate(outs):
        width = out.shape[1]
        source = w_hbm.at[:, pl.ds(start, width)]
        copies.append(pltpu.make_async_copy(source, out, sems.at[i]))
        start += width
    for copy in copies:
        copy.start()
    for copy in copies:
        copy.wait()


def load_call(weight, cuts):
    depth = weight.shape[0]
    widths = [stop - start for start, stop in zip(cuts, cuts[1:])]
    return pl.pallas_call(
        functools.partial(load_kernel, cuts[0]),
        out_shape=[pltpu.VMEM((depth, width), weight.dtype) for width in widths],
        in_specs=[ANY],
        out_specs=[VMEM] * len(widths),
        scratch_shapes=[pltpu.SemaphoreType.DMA((len(widths),))],
        cost_estimate=pl.CostEstimate(
            flops=0,
            transcendentals=0,
            bytes_accessed=2 * depth * (cuts[-1] - cuts[0]),
        ),
        compiler_params=pltpu.CompilerParams(vmem_limit_bytes=MIB),
        name="load",
    )(weight)


def in_hbm(x):
    return pltpu.with_memory_space_constraint(x, pltpu.HBM)


def query_doc(docs_ref, me):
    docs = docs_ref[...]
    own = lax.broadcasted_iota(jnp.int32, (docs.shape[0], HD), 0) == me
    column = lax.dot_general(
        docs,
        own.astype(jnp.float32),
        (((0,), (0,)), ((), ())),
        preferred_element_type=jnp.float32,
    )
    return column[:, :1]


def key_doc(docs_ref, block, me):
    row = docs_ref[pl.ds(jnp.maximum(block, 0), 1), :]
    return jnp.where((block >= 0) & (block <= me), row, -1.0)


def scores_of(queries, keys):
    return lax.dot_general(
        queries, keys, (((1,), (1,)), ((), ())), preferred_element_type=jnp.float32
    )


def with_ones(values):
    return jnp.concatenate([values, jnp.ones_like(values)], axis=1)


def early_kernel(kv_local, group, count, step, *refs):
    q_ref, docs_ref = refs[:2]
    blocks = refs[2 : 2 + count]
    acc_ref, top_ref, sum_ref, last_bias_ref = refs[2 + count : 6 + count]
    bias_ref, s_ref, p_ref = refs[6 + count :]
    tokens = q_ref.shape[0]
    me = lax.axis_index("seq")
    row, col = me // 2, me % 2
    docs = []
    for i in range(count):
        block = me - i if i % 2 == 0 else (row - i // 2) * 2 + 1 - col
        docs.append(key_doc(docs_ref, block, me))
    own_doc = query_doc(docs_ref, me)
    far = key_doc(docs_ref, (row - count // 2) * 2 + 1 - col, me)
    last_bias_ref[...] = jnp.where(own_doc == far, 0.0, -jnp.inf)
    allowed = own_doc == jnp.concatenate(docs, axis=1)
    key_at = lax.broadcasted_iota(jnp.int32, (tokens, count * tokens), 1)
    query_at = lax.broadcasted_iota(jnp.int32, (tokens, count * tokens), 0)
    allowed = allowed & ((key_at <= query_at) | (key_at >= tokens))
    bias_ref[...] = jnp.where(allowed, 0.0, -jnp.inf)
    keys, values = [], []
    for h in range(kv_local):
        at = pl.ds(2 * h * HD, HD)
        keys.append(jnp.concatenate([b[:, at] for b in blocks], axis=0))
        at = pl.ds((2 * h + 1) * HD, HD)
        values.append(with_ones(jnp.concatenate([b[:, at] for b in blocks], axis=0)))

    def score(head):
        s_ref[head] = scores_of(q_ref[:, pl.ds(head * HD, HD)], keys[head // group])

    def soften(head):
        for r in range(0, tokens, step):
            at = pl.ds(r, step)
            scores = s_ref[head, at, :] * SCALE + bias_ref[at, :]
            top = jnp.max(scores, axis=-1, keepdims=True)
            p_ref[head, at, :] = jnp.exp2(scores - top).astype(jnp.bfloat16)
            into = pl.ds(head * tokens + r, step)
            top_ref[into, :] = jnp.broadcast_to(top, (step, HD))

    def add_up(head):
        both = jnp.dot(
            p_ref[head], values[head // group], preferred_element_type=jnp.float32
        )
        into = pl.ds(head * tokens, tokens)
        acc_ref[into, :] = both[:, :HD]
        sum_ref[into, :] = both[:, HD:]

    heads = kv_local * group
    score(0)
    for head in range(heads):
        if head + 1 < heads:
            score(head + 1)
        soften(head)
        if head:
            add_up(head - 1)
    add_up(heads - 1)


def project(context_ref, first, w_ref, send_ref, keep_ref, part, top=0, more_ref=None):
    step = 256
    count = keep_ref.shape[0] // part
    for c in range(0, w_ref.shape[1], step):
        at = pl.ds(c, step)
        rows = jnp.dot(
            context_ref[pl.ds(first, 2 * count * part), :],
            w_ref[pl.ds(top, context_ref.shape[1]), at],
            preferred_element_type=jnp.float32,
        )
        if more_ref is not None:
            rows = rows + more_ref[:, at]
        rows = rows.astype(jnp.bfloat16)
        for i in range(count):
            into = pl.ds(i * part, part)
            keep_ref[into, at] = rows[2 * i * part : (2 * i + 1) * part]
            send_ref[into, at] = rows[(2 * i + 1) * part : (2 * i + 2) * part]


def late_kernel(h, kv_local, group, part, step, *refs):
    q_ref, bias_ref, block, acc_ref, top_ref, sum_ref, w_ref = refs[:7]
    context_ref, here_ref, s_ref, p_ref, rescale_ref = refs[-5:]
    refs = refs[7:-5]
    tokens = q_ref.shape[0]
    rank, chips = lax.axis_index("tp"), lax.axis_size("tp") // 2
    keys, values = block[:, pl.ds(0, HD)], with_ones(block[:, pl.ds(HD, HD)])

    def score(g):
        cols = pl.ds((h * group + g) * HD, HD)
        s_ref[g] = scores_of(q_ref[:, cols], keys)

    def soften(g):
        for r in range(0, tokens, step):
            at = pl.ds(r, step)
            scores = s_ref[g, at, :] * SCALE + bias_ref[at, :]
            old = top_ref[pl.ds((h * group + g) * tokens + r, step), :]
            new = jnp.maximum(old, jnp.max(scores, axis=-1, keepdims=True))
            p_ref[g, at, :] = jnp.exp2(scores - new[:, :1]).astype(jnp.bfloat16)
            rescale_ref[g, at, :] = jnp.exp2(old - new)

    def add_up(g):
        at = pl.ds((h * group + g) * tokens, tokens)
        added = jnp.dot(p_ref[g], values, preferred_element_type=jnp.float32)
        rescale = rescale_ref[g]
        total = sum_ref[at, :] * rescale + added[:, HD:]
        context = (acc_ref[at, :] * rescale + added[:, :HD]) / total
        context_ref[:, pl.ds(g * HD, HD)] = context.astype(jnp.bfloat16)

    score(0)
    for g in range(group):
        if g + 1 < group:
            score(g + 1)
        soften(g)
        if g:
            add_up(g - 1)
    add_up(group - 1)
    at = 0
    for distance in range(1, chips + 1):
        base = lax.rem(rank // 2 + distance, chips) * 2
        for core in (rank % 2, 1 - rank % 2):
            first = pl.multiple_of((base + core) * part, 8)
            here_ref[pl.ds(at, part), :] = context_ref[pl.ds(first, part), :]
            at += part
    depth_of = group * HD
    top = h * depth_of
    more_ref, before_ref = refs[:2] if h else (None, None)
    if h < kv_local - 1:
        part_ref, out_ref = refs[-2:]
        rows = part_ref.shape[0]
        step = 256
        for c in range(0, w_ref.shape[1], step):
            cols = pl.ds(c, step)
            product = jnp.dot(
                here_ref[pl.ds(0, rows), :],
                w_ref[pl.ds(top, depth_of), cols],
                preferred_element_type=jnp.float32,
            )
            part_ref[:, cols] = product if more_ref is None else product + more_ref[:, cols]
    else:
        send_ref, keep_ref, out_ref = refs[-3:]
        project(here_ref, 0, w_ref, send_ref, keep_ref, part, top, more_ref)
    out_ref[:, pl.ds(top, depth_of)] = here_ref[...]
    if h:
        out_ref[:, pl.ds(0, top)] = before_ref[...]


def project_kernel(part, first, context_ref, *refs):
    *weights, send_ref, keep_ref = refs
    start = 0
    for w_ref in weights:
        cols = pl.ds(start, w_ref.shape[1])
        send, keep = send_ref.at[:, cols], keep_ref.at[:, cols]
        project(context_ref, first, w_ref, send, keep, part)
        start += w_ref.shape[1]


def project_call(context, weights, part, first, rows):
    depth = context.shape[1]
    width = sum(weight.shape[1] for weight in weights)
    out = jax.ShapeDtypeStruct((rows // 2, width), jnp.bfloat16)
    return pl.pallas_call(
        functools.partial(project_kernel, part, first),
        out_shape=(out, out),
        in_specs=[VMEM] * (1 + len(weights)),
        out_specs=(VMEM, VMEM),
        cost_estimate=pl.CostEstimate(
            flops=2 * rows * depth * width,
            transcendentals=0,
            bytes_accessed=2 * depth * width,
        ),
        compiler_params=pltpu.CompilerParams(vmem_limit_bytes=PROJ * MIB),
        name="project_rest",
    )(context, *weights)


def finish_kernel(starts, kept_ref, received_ref, *refs):
    n = len(starts)
    *arrived, out_hbm = refs[: -n - 1]
    chunks, sems = refs[-n - 1 : -1], refs[-1]
    each = len(arrived) // n
    copies = []
    for i, start in enumerate(starts):
        cols = pl.ds(start, chunks[i].shape[1])
        total = kept_ref[:, cols].astype(jnp.float32)
        total = total + received_ref[:, cols].astype(jnp.float32)
        for ref in arrived[i * each : (i + 1) * each]:
            total = total + ref[...].astype(jnp.float32)
        chunks[i][...] = total.astype(jnp.bfloat16)
        copies.append(pltpu.make_async_copy(chunks[i], out_hbm.at[:, cols], sems.at[i]))
        copies[-1].start()
    for copy in copies:
        copy.wait()


def finish_call(kept, received, arrived, starts, out=None):
    flat = [block for blocks in arrived for block in blocks]
    n = len(starts)
    kernel = functools.partial(finish_kernel, starts)
    if out is not None:

        def kernel(kept_ref, received_ref, *refs):
            blocks, rest = refs[: len(flat)], refs[len(flat) + 1 :]
            finish_kernel(starts, kept_ref, received_ref, *blocks, *rest)

    return pl.pallas_call(
        kernel,
        out_shape=jax.ShapeDtypeStruct(kept.shape, kept.dtype),
        in_specs=[VMEM] * (2 + len(flat)) + [ANY] * (out is not None),
        out_specs=ANY,
        scratch_shapes=[pltpu.VMEM(blocks[0].shape, kept.dtype) for blocks in arrived]
        + [pltpu.SemaphoreType.DMA((n,))],
        input_output_aliases={} if out is None else {2 + len(flat): 0},
        cost_estimate=pl.CostEstimate(
            flops=4 * kept.size, transcendentals=0, bytes_accessed=4 * kept.size
        ),
        compiler_params=pltpu.CompilerParams(vmem_limit_bytes=4 * MIB),
        name="finish",
    )(kept, received, *flat, *([] if out is None else [out]))


def layer(query_rows, key_rows, value_rows, document_ids, output_weight):
    tokens = query_rows.shape[0]
    kv_local = key_rows.shape[1] // HD
    group = HEADS // KV
    width = query_rows.shape[1]
    model = output_weight.shape[1]
    seq, tp = lax.axis_size("seq"), lax.axis_size("tp")
    part = tokens // tp
    chips = tp // 2
    reach = min(12, seq // 2)
    depth = (reach + 1) // 2
    route = routes(seq, tp, depth)
    odd_row = (lax.axis_index("seq") // 2) % 2 == 1

    def send(x, name, step):
        return lax.ppermute(x, AXES, route[name, step])

    own = pl.pallas_call(
        join_kernel,
        out_shape=pltpu.VMEM((tokens, 2 * kv_local * HD), jnp.bfloat16),
        in_specs=[ANY, ANY],
        out_specs=VMEM,
        scratch_shapes=[pltpu.SemaphoreType.DMA((2 * kv_local,))],
        compiler_params=pltpu.CompilerParams(vmem_limit_bytes=2 * MIB),
        name="join",
    )(in_hbm(key_rows), in_hbm(value_rows))
    docs = document_ids.astype(jnp.float32).reshape(seq, tokens)
    cuts = [model * n // 32 for n in (0, *CUTS)]
    near = model * NEAR // 32
    weight = in_hbm(output_weight)
    first, *middle = load_call(weight, (0, cuts[1], near))
    *rest, third = load_call(weight, (near, *cuts[2:4]))
    weights = [[first], middle + rest, [third]]
    weights.append(load_call(weight, cuts[3:]))
    even, odd = send(own, "even", 1), send(own, "odd", 1)
    blocks = [own, send(own, "col", 0)]
    even, odd, docs = lax.optimization_barrier((even, odd, docs))
    for distance in range(1, depth + 1):
        blocks.append(jnp.where(odd_row, even, odd))
        if distance < depth:
            even, odd = (
                send(odd, "even", distance + 1),
                send(even, "odd", distance + 1),
            )
        if distance < depth:
            blocks.append(send(blocks[-1], "col", distance))
    last_blocks = []
    for h in range(kv_local):
        piece = blocks[-1][:, 2 * h * HD : 2 * (h + 1) * HD]
        last_blocks.append(lax.ppermute(piece, AXES, route["col", depth]))
    count = len(blocks)

    stacked = group * tokens
    state = jax.ShapeDtypeStruct((kv_local * stacked, HD), jnp.float32)
    early = pl.pallas_call(
        functools.partial(early_kernel, kv_local, group, count, 64),
        out_shape=(
            state,
            state,
            state,
            jax.ShapeDtypeStruct((tokens, tokens), jnp.float32),
        ),
        in_specs=[VMEM] * (2 + count),
        out_specs=(VMEM,) * 4,
        scratch_shapes=[
            pltpu.VMEM((tokens, count * tokens), jnp.float32),
            pltpu.VMEM((kv_local * group, tokens, count * tokens), jnp.float32),
            pltpu.VMEM((kv_local * group, tokens, count * tokens), jnp.bfloat16),
        ],
        cost_estimate=pl.CostEstimate(
            flops=4 * tokens * tokens * count * width,
            transcendentals=tokens * tokens * count * width // HD,
            bytes_accessed=4 * tokens * width,
        ),
        compiler_params=pltpu.CompilerParams(vmem_limit_bytes=EARLY * MIB),
        name="attend_early",
    )
    acc, top, total, bias = early(query_rows, docs, *blocks)

    remote = (chips - 1) * part
    out = jax.ShapeDtypeStruct((remote, cuts[1]), jnp.bfloat16)
    share = group * HD
    so_far = ()
    for h, last_block in enumerate(last_blocks):
        context_shape = jax.ShapeDtypeStruct((tokens, (h + 1) * share), jnp.bfloat16)
        if h < kv_local - 1:
            product = jax.ShapeDtypeStruct((2 * remote, cuts[1]), jnp.float32)
            shapes = (product, context_shape)
        else:
            shapes = (out, out, context_shape)
        so_far = pl.pallas_call(
            functools.partial(late_kernel, h, kv_local, group, part, 64),
            out_shape=shapes,
            in_specs=[VMEM] * (7 + len(so_far)),
            out_specs=(VMEM,) * len(shapes),
            scratch_shapes=[
                pltpu.VMEM((tokens, share), jnp.bfloat16),
                pltpu.VMEM((tokens, share), jnp.bfloat16),
                pltpu.VMEM((group, tokens, tokens), jnp.float32),
                pltpu.VMEM((group, tokens, tokens), jnp.bfloat16),
                pltpu.VMEM((group, tokens, HD), jnp.float32),
            ],
            cost_estimate=pl.CostEstimate(
                flops=4 * tokens * tokens * share + 4 * remote * share * cuts[1],
                transcendentals=tokens * tokens * group,
                bytes_accessed=4 * tokens * share + 2 * share * cuts[1],
            ),
            compiler_params=pltpu.CompilerParams(vmem_limit_bytes=LATE * MIB),
            name="attend_late",
        )(query_rows, bias, last_block, acc, top, total, first, *so_far)
    sent, kept, context = so_far

    arrived = []
    for i, weight in enumerate(weights):
        if i:
            sent, kept = project_call(context, weight, part, 0, 2 * remote)
        received = send(sent, "core", i)
        moved = kept.astype(jnp.float32) + received.astype(jnp.float32)
        moved = moved.astype(jnp.bfloat16)
        arrived.append([])
        for distance in range(1, chips):
            at = (distance - 1) * part
            block = lax.ppermute(
                moved[at : at + part], AXES, y_route(seq, tp, distance)
            )
            arrived[-1].append(block)
    every = [weight for weights_of in weights for weight in weights_of]
    sent, kept = project_call(context, every, part, 2 * remote, 2 * part)
    received = send(sent, "core", len(CUTS))
    out = finish_call(kept, received, arrived[:-1], cuts[:-2])
    return finish_call(kept, received, arrived[-1:], cuts[-2:-1], out)


def solution(mesh):
    in_specs = (P("seq", "tp"), P("seq", "tp"), P("seq", "tp"), P(), P("tp", None))
    out_specs = P(("seq", "tp"), None)
    return jax.shard_map(
        layer, mesh=mesh, in_specs=in_specs, out_specs=out_specs, check_vma=False
    )
```
